256 devices in a mesh: grp: 4 (over y), dev: 64 (over x, z, core).
Axes of the slice: x: 4, y: 4, z: 8, core: 2. Of those that a mesh axis runs over, the one named last changes fastest.
Arguments:
- pool_rows: bfloat16 [262144, 1024], P(('grp', 'dev')), may hold values from -6 to 6
- sample_index: int32 [262144], P(('grp', 'dev')), may hold values from 0 to 262143, as said below
- cluster_id: int32 [262144], P(('grp', 'dev')), may hold values from 0 to 511, as said below
- child_id: int32 [262144], P(('grp', 'dev')), may hold values from 0 to 7
- old_centroids: float32 [512, 8, 1024], P('dev'), may hold values from -6 to 6
Outputs:
- centroids: float32 [512, 8, 1024], P('dev')
- child_counts: int32 [512, 8], P('dev')
The draws below stay inside these ranges and needn't reach their ends.
Inputs may be any that keep to these rules, and one draw needn't show every extreme that they name: Sample i takes a pool row of its own aligned block of 1024 rows: sample_index[i] // 1024 == i // 1024. `cluster_id`: in each aligned block of 1024 samples (the rows of one device) the 2 clusters o * 2 to o * 2 + 1 of any owner o are named at most 8 times together, and one cluster, the same in every block, is named exactly 8 times in every block.
All inputs are finite; a program needn't handle non-finite values.
Results may differ from the reference program's by a relative error of at most 0.0003.
Values may be sent and summed in bfloat16 or wider, within the bound.
A program may use at most 64 MiB of HBM per device.

```python
import jax
import jax.numpy as jnp
from jax import lax

D = 1024
KC = 8
CL_DEV = 2
R_DEV = 1024
CLUSTERS = 512
ROWS = 262144
MOST = 8


def shuffle_row(subkey, values):
    return jax.random.permutation(subkey, values)


def draw_cluster_id(key, part):
    blocks = ROWS // R_DEV
    holder_tally_overall = CLUSTERS // CL_DEV
    slots = holder_tally_overall * MOST
    full_key = jax.random.fold_in(key, 11)
    favour_noise_seed = jax.random.fold_in(key, 12)
    noise_key = jax.random.fold_in(key, 13)
    order_key = jax.random.fold_in(key, 14)
    pick_key = jax.random.fold_in(key, 15)
    favoured = jax.random.randint(full_key, (), 0, CLUSTERS)
    favourite_holder_position = favoured // CL_DEV
    holder_advantage = jax.random.randint(favour_noise_seed, (holder_tally_overall,), 0, 4)
    uniform_perturbation = jax.random.randint(noise_key, (blocks, slots), 0, 16384)
    holder_table = (jnp.arange(slots) // MOST).astype(jnp.int32)
    holder_merit = uniform_perturbation + holder_advantage[holder_table][None, :] * 4096 + jnp.where(holder_table == favourite_holder_position, 65536, 0)[None, :]
    holder_merit = (holder_merit * slots + jnp.arange(slots)[None, :]).astype(jnp.int32)
    unused, chosen = lax.top_k(holder_merit, R_DEV)
    keys = jax.random.split(order_key, blocks)
    mixed = jax.vmap(shuffle_row)(keys, chosen.astype(jnp.int32))
    owner = (mixed // MOST).astype(jnp.int32)
    pick = jax.random.randint(pick_key, (blocks, R_DEV), 0, CL_DEV)
    cluster = owner * CL_DEV + pick
    cluster = jnp.where(owner == favourite_holder_position, favoured, cluster)
    return cluster.reshape(-1).astype(jnp.int32)


def draw_sample_index(key, part):
    offset_key = jax.random.fold_in(key, 21)
    within = jax.random.randint(offset_key, (ROWS,), 0, R_DEV)
    base = jnp.arange(ROWS) // R_DEV * R_DEV
    return (base + within).astype(jnp.int32)


def place_ends(entries, rng, low, top_value):
    longest = entries.shape.index(max(entries.shape))
    spots = []
    for shift in (0, 1):
        where = [jax.random.randint(jax.random.fold_in(rng, axis), (), 0, length) for axis, length in enumerate(entries.shape)]
        where[longest] = (where[longest] + shift) % entries.shape[longest]
        spots.append(tuple(where))
    return entries.at[spots[0]].set(low).at[spots[1]].set(top_value)


def shard_levels(key, shape, shards, least, largest):
    def one(dim, blocks):
        draws = jax.random.uniform(jax.random.fold_in(jax.random.fold_in(key, 6), dim), (blocks,), jnp.float32, least / len(shards), largest / len(shards))
        return jnp.repeat(jnp.exp(draws), shape[dim] // blocks).reshape((-1,) + (1,) * (len(shape) - dim - 1))

    gain = one(*shards[0])
    for cut in shards[1:]:
        gain = gain * one(*cut)
    return gain


def scatter_about(stream_key, dims, spread, most, pieces=(), dtype=jnp.bfloat16):
    loudness = shard_levels(stream_key, dims, pieces, -0.22, 0.18) if pieces else 1.0
    drawn = jax.random.normal(stream_key, dims, jnp.float32) * spread * loudness
    return jnp.minimum(jnp.maximum(drawn, -most), most).astype(dtype)


def setup_inputs(seed: int = 0) -> dict:
    arg_keys = jax.random.split(jax.random.key(seed), 6)
    pool_rows = scatter_about(arg_keys[0], (ROWS, D), 1.0, 6.0, ((0, 256),))
    sample_index = draw_sample_index(jax.random.fold_in(arg_keys[5], 71), 0)
    cluster_id = draw_cluster_id(jax.random.fold_in(arg_keys[5], 71), 0)
    child_id = place_ends(jax.random.randint(arg_keys[3], (ROWS,), 0, KC), jax.random.fold_in(arg_keys[3], 1), 0, KC - 1).astype(jnp.int32)
    old_centroids = scatter_about(arg_keys[4], (CLUSTERS, KC, D), 1.0, 6.0, ((0, 64),), jnp.float32)
    return dict(pool_rows=pool_rows, sample_index=sample_index, cluster_id=cluster_id, child_id=child_id, old_centroids=old_centroids)


def reference(pool_rows, sample_index, cluster_id, child_id, old_centroids):
    blocks = ROWS // R_DEV
    segments = CLUSTERS * KC

    def add_block(carry, items):
        sums, counts = carry
        index_block, cluster_block, child_block = items
        rows = pool_rows[index_block].astype(jnp.float32)
        segment = (cluster_block * KC + child_block).astype(jnp.int32)
        sums = sums + jax.ops.segment_sum(rows, segment, num_segments=segments)
        ones = jnp.ones(segment.shape, jnp.int32)
        counts = counts + jax.ops.segment_sum(ones, segment, num_segments=segments)
        return (sums, counts), None

    initial = (jnp.zeros((segments, D), jnp.float32), jnp.zeros((segments,), jnp.int32))
    items = (sample_index.reshape(blocks, R_DEV), cluster_id.reshape(blocks, R_DEV), child_id.reshape(blocks, R_DEV))
    (sums, counts), unused = lax.scan(add_block, initial, items)
    child_counts = counts.reshape(CLUSTERS, KC)
    divisor = child_counts.astype(jnp.float32)[:, :, None] + 1.0
    centroids = (sums.reshape(CLUSTERS, KC, D) + old_centroids) / divisor
    return (centroids, child_counts)
```

```python
import functools

import jax
import jax.numpy as jnp
from jax import lax
from jax.experimental import pallas as pl
from jax.experimental.pallas import tpu as pltpu
from jax.sharding import PartitionSpec as P

MESH = pl.DeviceIdType.MESH
F32, BF16, I32 = jnp.float32, jnp.bfloat16, jnp.int32

NY, NX, NZ, NC = 4, 4, 8, 2
MEMBERS, SLOTS = 8, 32
BLOCK = MEMBERS * SLOTS
ROWS, WIDTH = 1024, 1024
HALF = WIDTH // 2
SEGS = 64
OWN = 16
AHEAD = 3


def kernel(
    pool_ref, index_ref, cluster_ref, child_ref, old_ref,
    out_ref, count_ref,
    slot_ref, values_ref, send, recv, lab_send, lab_recv,
    z_send, z_recv, total, part_recv, fresh,
    c_send, c_recv, c_mid, c_mid_recv, c_last, c_last_recv,
    data_ss, data_rs, lab_ss, lab_rs, z_ss, z_rs, part_ss, part_rs,
    gather_ss, gather_rs, c_ss, c_rs, own_sem,
):
    y = lax.axis_index("grp")
    d = lax.axis_index("dev")
    x, z, c = d // (NZ * NC), (d // NC) % NZ, d % NC

    def dev(x_, z_, c_):
        return (x_ * NZ + z_) * NC + c_

    def member(h, r):
        e = ((x if h == 0 else y) * NC + c + r) % MEMBERS
        if h == 0:
            return (y, dev(e // NC, z, e % NC))
        return (e // NC, dev(x, z, e % NC))

    def along_z(step):
        return (y, dev(x, (z + step + NZ) % NZ, c))

    def other(h, i):
        if h == 0:
            return ((y + i) % NY, d)
        return (y, dev((x + i) % NX, z, c))

    def push(src, dst, ss, rs, to):
        pltpu.make_async_remote_copy(
            src_ref=src, dst_ref=dst, send_sem=ss, recv_sem=rs, device_id=to, device_id_type=MESH
        ).start()

    def await_bytes(ref, sem):
        pltpu.make_async_copy(ref, ref, sem).wait()

    barrier = pltpu.get_barrier_semaphore()
    greeted = [member(h, r) for h in (0, 1) for r in range(1, MEMBERS)]
    greeted += [along_z(s) for s in range(1, NZ)]
    for to in greeted:
        pl.semaphore_signal(barrier, inc=1, device_id=to, device_id_type=MESH)

    cluster, child = cluster_ref[...], child_ref[...]
    index = index_ref[...] & (ROWS - 1)
    cx, cz, cc, cj = cluster >> 7, (cluster >> 4) & 7, (cluster >> 3) & 1, cluster & 7
    zr = (cz - z + NZ) & (NZ - 1)
    pos = jnp.where(zr >= 4, 2 * (zr - 4), 7 - 2 * zr)
    rx = (cx * NC + cc - (x * NC + c) + MEMBERS) & (MEMBERS - 1)
    ry = ((cj >> 1) * NC + cc - (y * NC + c) + MEMBERS) & (MEMBERS - 1)
    label_x = cj * 8 + child
    label_y = cx * OWN + (cj & 1) * 8 + child
    cat_x = pos * MEMBERS + rx
    cat_y = pos * MEMBERS + ry + 64

    sub = lax.broadcasted_iota(I32, (128, 128), 0)
    lane = lax.broadcasted_iota(I32, (128, 128), 1)
    before = jnp.concatenate(
        [jnp.where(sub <= lane, 1.0, 0.0), jnp.ones((128, 128), F32)], axis=1
    ).astype(BF16)
    hits = []
    for b in range(ROWS // 128):
        at = slice(b * 128, (b + 1) * 128)
        hits.append((sub == cat_x[:, at]) | (sub == cat_y[:, at]))
    stacked = jnp.concatenate([jnp.where(m, 1.0, 0.0).astype(BF16) for m in hits], axis=0)
    ranks = jnp.dot(stacked, before, preferred_element_type=F32)
    base = ((sub & 63) * SLOTS - 1).astype(F32)
    for b in range(ROWS // 128):
        at = slice(b * 128, (b + 1) * 128)
        here = ranks[b * 128 : (b + 1) * 128]
        chosen = jnp.where(hits[b], here[:, :128] + base, 0.0)
        slot_ref[0, :, at] = jnp.sum(chosen[:64], axis=0, keepdims=True).astype(I32)
        slot_ref[1, :, at] = jnp.sum(chosen[64:], axis=0, keepdims=True).astype(I32)
        base = base + here[:, 128:]

    values = jnp.concatenate(
        [index >> 5, index & 31, label_x + 1, label_y + 1, jnp.zeros((4, ROWS), I32)], axis=0
    ).astype(F32)
    values = jnp.concatenate([values, jnp.zeros((120, ROWS), F32)], axis=0)
    values_ref[...] = values.T.astype(BF16)

    sub_block = lax.broadcasted_iota(I32, (BLOCK, ROWS), 0)
    lane_block = lax.broadcasted_iota(I32, (BLOCK, ROWS), 1)
    lab_lane = lax.broadcasted_iota(I32, (1, BLOCK), 1)

    def place(p, h):
        pick = jnp.where(sub_block == slot_ref[h] - p * BLOCK, 1.0, 0.0).astype(BF16)
        found = jnp.dot(pick, values_ref[...], preferred_element_type=F32)
        row = (found[:, 0:1] * 32.0 + found[:, 1:2]).astype(I32)
        labels = found.T[2 + h : 3 + h].astype(I32)
        take = jnp.where(lane_block == row, 1.0, 0.0).astype(BF16)
        rows = jnp.dot(
            take, pool_ref[:, h * HALF : (h + 1) * HALF], preferred_element_type=F32
        ).astype(BF16)
        recv[h, p, 0] = rows[:SLOTS]
        send[h, p, pl.ds(1, MEMBERS - 1)] = rows[SLOTS:].reshape(MEMBERS - 1, SLOTS, HALF)
        for r in range(MEMBERS):
            mine = jnp.where((lab_lane >> 5) == r, labels, 0)
            if r == 0:
                lab_recv[h, p, 0] = mine
            else:
                lab_send[h, p, r] = mine

    def dispatch(p, h):
        for r in range(1, MEMBERS):
            to = member(h, r)
            push(lab_send.at[h, p, r], lab_recv.at[h, p, r], lab_ss.at[h, p], lab_rs.at[h, p], to)
            push(send.at[h, p, r], recv.at[h, p, r], data_ss.at[h, p], data_rs.at[h, p], to)

    seg = lax.broadcasted_iota(I32, (SEGS, BLOCK), 0) + 1

    def reduce_rows(p, h):
        await_bytes(lab_recv.at[h, p, pl.ds(1, MEMBERS - 1)], lab_rs.at[h, p])
        await_bytes(recv.at[h, p, pl.ds(1, MEMBERS - 1)], data_rs.at[h, p])
        labels = lab_recv[h, p, 0]
        for r in range(1, MEMBERS):
            labels = labels + lab_recv[h, p, r]
        onehot = jnp.where(seg == labels, 1.0, 0.0).astype(BF16)
        return jnp.dot(onehot, recv[h, p].reshape(BLOCK, HALF), preferred_element_type=F32)

    UP, DOWN = 0, 1

    def forward(h, way, k, partial):
        z_send[h, way, k] = partial
        to = along_z(1 if way == UP else -1)
        push(z_send.at[h, way, k], z_recv.at[h, way, k], z_ss.at[h, way, k], z_rs.at[h, way, k], to)

    def incoming(h, way, k):
        await_bytes(z_recv.at[h, way, k], z_rs.at[h, way, k])
        return z_recv[h, way, k]

    pl.semaphore_wait(barrier, len(greeted))

    def first(p, carry):
        for h in (0, 1):
            place(p, h)
            dispatch(p, h)
        return carry

    lax.fori_loop(0, AHEAD, first, 0)

    place_row = rx * NZ + cz
    a_hot = jnp.where(lax.broadcasted_iota(I32, (64, ROWS), 0) == place_row, 1.0, 0.0).astype(BF16)
    b_hot = jnp.where(lax.broadcasted_iota(I32, (128, ROWS), 0) == label_x, 1.0, 0.0).astype(BF16)
    tally = lax.dot_general(a_hot, b_hot, (((1,), (1,)), ((), ())), preferred_element_type=F32)
    c_send[...] = tally.reshape(MEMBERS, NZ, 128)
    for r in range(1, MEMBERS):
        push(c_send.at[r], c_recv.at[r], c_ss.at[0], c_rs.at[0], member(0, r))

    forward(0, UP, 3, reduce_rows(0, 0))
    forward(1, DOWN, 3, reduce_rows(0, 1))

    await_bytes(c_recv.at[pl.ds(1, MEMBERS - 1)], c_rs.at[0])
    group_count = c_send[0]
    for r in range(1, MEMBERS):
        group_count = group_count + c_recv[r]
    c_mid[...] = group_count
    for s in range(1, NZ):
        push(c_mid, c_mid_recv.at[s], c_ss.at[1], c_rs.at[1], along_z(s))

    def pair(i, carry):
        k = 2 - i
        for way in (UP, DOWN):
            p = 1 + 2 * i + way
            for h in (0, 1):
                partial = reduce_rows(p, h)
                if way == h:
                    partial = partial + incoming(h, way, k + 1)
                else:
                    z_send[h, way, k] = partial

                    @pl.when(i > 0)
                    def _():
                        z_send[h, way, k] += incoming(h, way, k + 1)

                    partial = None
                if partial is not None:
                    z_send[h, way, k] = partial
                to = along_z(1 if way == UP else -1)
                push(z_send.at[h, way, k], z_recv.at[h, way, k], z_ss.at[h, way, k], z_rs.at[h, way, k], to)

            @pl.when(p + AHEAD - 1 < 8)
            def _():
                first(p + AHEAD - 1, 0)

        return carry

    lax.fori_loop(0, 3, pair, 0)

    await_bytes(c_mid_recv.at[pl.ds(1, NZ - 1)], c_rs.at[1])
    plane_count = c_mid[...]
    for s in range(1, NZ):
        plane_count = plane_count + c_mid_recv[s]
    c_last[...] = plane_count
    for i in range(1, NY):
        push(c_last, c_last_recv.at[i], c_ss.at[2], c_rs.at[2], other(0, i))

    for h in (0, 1):
        own = reduce_rows(7, h)
        own = own + incoming(h, UP, 0)
        own = own + incoming(h, DOWN, 0)
        total[h] = own.reshape(4, OWN, HALF)
        at = y if h == 0 else x
        for i in range(1, 4):
            push(total.at[h, (at + i) % 4], part_recv.at[h, i], part_ss.at[h], part_rs.at[h], other(h, i))

    await_bytes(c_last_recv.at[pl.ds(1, NY - 1)], c_rs.at[2])
    all_count = c_last[...]
    for i in range(1, NY):
        all_count = all_count + c_last_recv[i]
    row_of = lax.broadcasted_iota(I32, (NZ, 128), 0)
    block_count = jnp.sum(jnp.where(row_of == z, all_count, 0.0), axis=0, keepdims=True)
    for j in range(8):
        count_ref[j : j + 1, :] = block_count[:, j * 8 : (j + 1) * 8].astype(I32)
    own_sub = lax.broadcasted_iota(I32, (OWN, 128), 0) + y * OWN
    own_lane = lax.broadcasted_iota(I32, (OWN, 128), 1)
    column = jnp.sum(jnp.where(own_sub == own_lane, block_count, 0.0), axis=1, keepdims=True)

    for h in (0, 1):
        at = y if h == 0 else x
        cols = pl.ds(h * HALF, HALF)
        await_bytes(part_recv.at[h, pl.ds(1, 3)], part_rs.at[h])
        mine = total[h, at]
        for i in range(1, 4):
            mine = mine + part_recv[h, i]
        old = old_ref[pl.ds(y * 2, 2), :, cols].reshape(OWN, HALF)
        fresh[:, :, cols] = ((mine + old) / (column + 1.0)).reshape(2, 8, HALF)
        src = fresh.at[:, :, cols]
        dst = out_ref.at[pl.ds(y * 2, 2), :, cols]
        for i in range(1, NY):
            push(src, dst, gather_ss.at[h], gather_rs.at[h], other(0, i))
        pltpu.make_async_copy(src, dst, own_sem.at[h]).start()

    for h in (0, 1):
        for p in range(8):
            await_bytes(lab_send.at[h, p, pl.ds(1, MEMBERS - 1)], lab_ss.at[h, p])
            await_bytes(send.at[h, p, pl.ds(1, MEMBERS - 1)], data_ss.at[h, p])
        for way in (UP, DOWN):
            for k in range(4 if way == h else 3):
                await_bytes(z_send.at[h, way, k], z_ss.at[h, way, k])
        await_bytes(part_recv.at[h, pl.ds(1, 3)], part_ss.at[h])
        cols = pl.ds(h * HALF, HALF)
        await_bytes(out_ref.at[pl.ds(0, 6), :, cols], gather_ss.at[h])
        await_bytes(out_ref.at[pl.ds(0, 6), :, cols], gather_rs.at[h])
        await_bytes(out_ref.at[pl.ds(0, 2), :, cols], own_sem.at[h])
    await_bytes(c_recv.at[pl.ds(1, MEMBERS - 1)], c_ss.at[0])
    await_bytes(c_mid_recv.at[pl.ds(1, NZ - 1)], c_ss.at[1])
    await_bytes(c_last_recv.at[pl.ds(1, NY - 1)], c_ss.at[2])


def per_device(pool_rows, sample_index, cluster_id, child_id, old_centroids):
    vmem = pl.BlockSpec(memory_space=pltpu.VMEM)
    dma = pltpu.SemaphoreType.DMA
    centroids, counts = pl.pallas_call(
        kernel,
        out_shape=(
            jax.ShapeDtypeStruct((8, 8, WIDTH), F32),
            jax.ShapeDtypeStruct((8, 8), I32),
        ),
        in_specs=[vmem] * 5,
        out_specs=(pl.BlockSpec(memory_space=pl.ANY), vmem),
        scratch_shapes=[
            pltpu.VMEM((2, 1, ROWS), I32),
            pltpu.VMEM((ROWS, 128), BF16),
            pltpu.VMEM((2, 8, MEMBERS, SLOTS, HALF), BF16),
            pltpu.VMEM((2, 8, MEMBERS, SLOTS, HALF), BF16),
            pltpu.VMEM((2, 8, MEMBERS, 1, BLOCK), I32),
            pltpu.VMEM((2, 8, MEMBERS, 1, BLOCK), I32),
            pltpu.VMEM((2, 2, 4, SEGS, HALF), F32),
            pltpu.VMEM((2, 2, 4, SEGS, HALF), F32),
            pltpu.VMEM((2, 4, OWN, HALF), F32),
            pltpu.VMEM((2, 4, OWN, HALF), F32),
            pltpu.VMEM((2, 8, WIDTH), F32),
            pltpu.VMEM((MEMBERS, NZ, 128), F32),
            pltpu.VMEM((MEMBERS, NZ, 128), F32),
            pltpu.VMEM((NZ, 128), F32),
            pltpu.VMEM((NZ, NZ, 128), F32),
            pltpu.VMEM((NZ, 128), F32),
            pltpu.VMEM((NY, NZ, 128), F32),
            dma((2, 8)), dma((2, 8)), dma((2, 8)), dma((2, 8)),
            dma((2, 2, 4)), dma((2, 2, 4)), dma((2,)), dma((2,)),
            dma((2,)), dma((2,)), dma((3,)), dma((3,)), dma((2,)),
        ],
        compiler_params=pltpu.CompilerParams(
            collective_id=0, has_side_effects=True, vmem_limit_bytes=48 << 20
        ),
    )(
        pool_rows,
        sample_index.reshape(1, ROWS),
        cluster_id.reshape(1, ROWS),
        child_id.reshape(1, ROWS),
        old_centroids,
    )
    return centroids, counts


def solution(mesh):
    placed = (
        P(("grp", "dev"), None),
        P(("grp", "dev")),
        P(("grp", "dev")),
        P(("grp", "dev")),
        P("dev", None, None),
    )
    return jax.shard_map(
        per_device,
        mesh=mesh,
        in_specs=placed,
        out_specs=(P("dev", None, None), P("dev", None)),
        check_vma=False,
    )
```

```python
import jax
import jax.numpy as jnp
from jax import lax
from jax.experimental import pallas as pl
from jax.experimental.pallas import tpu as pltpu
from jax.sharding import PartitionSpec as P

MESH = pl.DeviceIdType.MESH
F32, BF16, I32 = jnp.float32, jnp.bfloat16, jnp.int32

NY, NX, NZ, NC = 4, 4, 8, 2
MEMBERS, SLOTS = 8, 32
BLOCK = MEMBERS * SLOTS
ROWS, WIDTH = 1024, 1024
HALF = WIDTH // 2
SEGS = 64
OWN = 16
AHEAD = 3
PIECES = 2
PIECE = HALF // PIECES
LATE = 6


def kernel(
    pool_hbm, index_hbm, cluster_hbm, child_hbm, old_hbm,
    out_ref, count_ref,
    pool_ref, index_ref, cluster_ref, child_ref, old_ref,
    slot_ref, values_ref, send, recv, lab_send, lab_recv,
    z_send, z_recv, total, part_recv, fresh,
    c_send, c_recv, c_group, cz_send, cz_recv, c_last, c_last_recv,
    in_sem, data_ss, data_rs, lab_ss, lab_rs, z_ss, z_rs, part_ss, part_rs,
    gather_ss, gather_rs, c_ss, c_rs, cz_ss, cz_rs, own_sem, late_ss, late_rs, last_ss, last_rs,
):
    y = lax.axis_index("grp")
    d = lax.axis_index("dev")
    x, z, c = d // (NZ * NC), (d // NC) % NZ, d % NC

    def dev(x_, z_, c_):
        return (x_ * NZ + z_) * NC + c_

    def member(h, r):
        e = ((x if h == 0 else y) * NC + c + r) % MEMBERS
        if h == 0:
            return (y, dev(e // NC, z, e % NC))
        return (e // NC, dev(x, z, e % NC))

    def along_z(step):
        return (y, dev(x, (z + step + NZ) % NZ, c))

    def other(h, i):
        if h == 0:
            return ((y + i) % NY, d)
        return (y, dev((x + i) % NX, z, c))

    def push(src, dst, ss, rs, to):
        pltpu.make_async_remote_copy(
            src_ref=src, dst_ref=dst, send_sem=ss, recv_sem=rs, device_id=to, device_id_type=MESH
        ).start()

    def await_bytes(ref, sem):
        pltpu.make_async_copy(ref, ref, sem).wait()

    inputs = [
        pltpu.make_async_copy(src, dst, in_sem.at[i])
        for i, (src, dst) in enumerate(
            [(index_hbm, index_ref), (cluster_hbm, cluster_ref), (child_hbm, child_ref),
             (pool_hbm, pool_ref), (old_hbm, old_ref)]
        )
    ]
    for copy in inputs:
        copy.start()

    barrier = pltpu.get_barrier_semaphore()
    greeted = [member(h, r) for h in (0, 1) for r in range(1, MEMBERS)]
    greeted += [along_z(1), along_z(-1)]
    for to in greeted:
        pl.semaphore_signal(barrier, inc=1, device_id=to, device_id_type=MESH)

    for copy in inputs[:3]:
        copy.wait()
    cluster, child = cluster_ref[...], child_ref[...]
    index = index_ref[...] & (ROWS - 1)
    cx, cz, cc, cj = cluster >> 7, (cluster >> 4) & 7, (cluster >> 3) & 1, cluster & 7
    zr = (cz - z + NZ) & (NZ - 1)
    pos_x = jnp.where(zr >= 4, 2 * (zr - 4), 7 - 2 * zr)
    zr = (NZ - zr) & (NZ - 1)
    pos_y = jnp.where(zr >= 4, 2 * (zr - 4), 7 - 2 * zr)
    rx = (cx * NC + cc - (x * NC + c) + MEMBERS) & (MEMBERS - 1)
    ry = ((cj >> 1) * NC + cc - (y * NC + c) + MEMBERS) & (MEMBERS - 1)
    label_x = cj * 8 + child
    label_y = cx * OWN + (cj & 1) * 8 + child
    cat_x = pos_x * MEMBERS + rx
    cat_y = pos_y * MEMBERS + ry + 64

    sub = lax.broadcasted_iota(I32, (128, 128), 0)
    lane = lax.broadcasted_iota(I32, (128, 128), 1)
    before = jnp.concatenate(
        [jnp.where(sub <= lane, 1.0, 0.0), jnp.ones((128, 128), F32)], axis=1
    ).astype(BF16)
    hits = []
    for b in range(ROWS // 128):
        at = slice(b * 128, (b + 1) * 128)
        hits.append((sub == cat_x[:, at]) | (sub == cat_y[:, at]))
    stacked = jnp.concatenate([jnp.where(m, 1.0, 0.0).astype(BF16) for m in hits], axis=0)
    ranks = jnp.dot(stacked, before, preferred_element_type=F32)
    base = ((sub & 63) * SLOTS - 1).astype(F32)
    for b in range(ROWS // 128):
        at = slice(b * 128, (b + 1) * 128)
        here = ranks[b * 128 : (b + 1) * 128]
        chosen = jnp.where(hits[b], here[:, :128] + base, 0.0)
        slot_ref[0, :, at] = jnp.sum(chosen[:64], axis=0, keepdims=True).astype(I32)
        slot_ref[1, :, at] = jnp.sum(chosen[64:], axis=0, keepdims=True).astype(I32)
        base = base + here[:, 128:]

    values = jnp.concatenate(
        [index >> 5, index & 31, label_x + 1, label_y + 1, jnp.zeros((4, ROWS), I32)], axis=0
    ).astype(F32)
    values = jnp.concatenate([values, jnp.zeros((120, ROWS), F32)], axis=0)
    values_ref[...] = values.T.astype(BF16)

    sub_block = lax.broadcasted_iota(I32, (BLOCK, ROWS), 0)
    lane_block = lax.broadcasted_iota(I32, (BLOCK, ROWS), 1)
    lab_lane = lax.broadcasted_iota(I32, (1, BLOCK), 1)

    def place(p, h):
        pick = jnp.where(sub_block == slot_ref[h] - p * BLOCK, 1.0, 0.0).astype(BF16)
        found = jnp.dot(pick, values_ref[...], preferred_element_type=F32)
        row = (found[:, 0:1] * 32.0 + found[:, 1:2]).astype(I32)
        labels = found.T[2 + h : 3 + h].astype(I32)
        take = jnp.where(lane_block == row, 1.0, 0.0).astype(BF16)
        rows = jnp.dot(
            take, pool_ref[:, h * HALF : (h + 1) * HALF], preferred_element_type=F32
        ).astype(BF16)
        recv[h, p, 0] = rows[:SLOTS]
        send[h, p, pl.ds(1, MEMBERS - 1)] = rows[SLOTS:].reshape(MEMBERS - 1, SLOTS, HALF)
        for r in range(MEMBERS):
            mine = jnp.where((lab_lane >> 5) == r, labels, 0)
            if r == 0:
                lab_recv[h, p, 0] = mine
            else:
                lab_send[h, p, r] = mine

    def columns(q):
        return pl.ds(q * PIECE, PIECE)

    def dispatch(p, h):
        for r in range(1, MEMBERS):
            to = member(h, r)
            push(lab_send.at[h, p, r], lab_recv.at[h, p, r], lab_ss.at[h, p], lab_rs.at[h, p], to)
            push(send.at[h, p, r], recv.at[h, p, r], data_ss.at[h, p], data_rs.at[h, p], to)

    def dispatch_pieces(p, h):
        for q in range(PIECES):
            for r in range(1, MEMBERS):
                to = member(h, r)
                if q == 0:
                    push(lab_send.at[h, p, r], lab_recv.at[h, p, r], lab_ss.at[h, p], lab_rs.at[h, p], to)
                at = (h, p - LATE, q)
                push(
                    send.at[h, p, r, :, columns(q)], recv.at[h, p, r, :, columns(q)],
                    late_ss.at[at], late_rs.at[at], to,
                )

    seg = lax.broadcasted_iota(I32, (SEGS, BLOCK), 0) + 1

    def onehot_of(p, h):
        await_bytes(lab_recv.at[h, p, pl.ds(1, MEMBERS - 1)], lab_rs.at[h, p])
        labels = lab_recv[h, p, 0]
        for r in range(1, MEMBERS):
            labels = labels + lab_recv[h, p, r]
        return jnp.where(seg == labels, 1.0, 0.0).astype(BF16)

    def reduce_rows(p, h):
        onehot = onehot_of(p, h)
        await_bytes(recv.at[h, p, pl.ds(1, MEMBERS - 1)], data_rs.at[h, p])
        return jnp.dot(onehot, recv[h, p].reshape(BLOCK, HALF), preferred_element_type=F32)

    def reduce_piece(onehot, p, h, q):
        await_bytes(recv.at[h, p, pl.ds(1, MEMBERS - 1), :, columns(q)], late_rs.at[h, p - LATE, q])
        rows = recv[h, p, :, :, columns(q)].reshape(BLOCK, PIECE)
        return jnp.dot(onehot, rows, preferred_element_type=F32)

    def onward(h, way):
        return along_z(1 if way == h else -1)

    def forward(h, way, k):
        push(
            z_send.at[h, way, k], z_recv.at[h, way, k], z_ss.at[h, way, k], z_rs.at[h, way, k],
            onward(h, way),
        )

    def incoming(h, way, k):
        await_bytes(z_recv.at[h, way, k], z_rs.at[h, way, k])
        return z_recv[h, way, k]

    def forward_count(way, k):
        push(
            cz_send.at[way, k], cz_recv.at[way, k], cz_ss.at[way, k], cz_rs.at[way, k],
            onward(0, way),
        )

    def incoming_count(way, k):
        await_bytes(cz_recv.at[way, k], cz_rs.at[way, k])
        return cz_recv[way, k]

    def count_of(steps):
        return c_group[pl.ds((z + steps + NZ) % NZ, 1), :]

    def first(p, carry):
        for h in (0, 1):
            place(p, h)

            @pl.when(p < LATE)
            def _():
                dispatch(p, h)

            @pl.when(p >= LATE)
            def _():
                dispatch_pieces(p, h)

        return carry

    def opening(p, carry):
        for h in (0, 1):
            place(p, h)
            dispatch(p, h)
        return carry

    inputs[3].wait()
    pl.semaphore_wait(barrier, len(greeted))
    lax.fori_loop(0, 1, opening, 0)

    place_row = rx * NZ + cz
    a_hot = jnp.where(lax.broadcasted_iota(I32, (64, ROWS), 0) == place_row, 1.0, 0.0).astype(BF16)
    b_hot = jnp.where(lax.broadcasted_iota(I32, (128, ROWS), 0) == label_x, 1.0, 0.0).astype(BF16)
    tally = lax.dot_general(a_hot, b_hot, (((1,), (1,)), ((), ())), preferred_element_type=F32)
    c_send[...] = tally.reshape(MEMBERS, NZ, 128)
    for r in range(1, MEMBERS):
        push(c_send.at[r], c_recv.at[r], c_ss.at[0], c_rs.at[0], member(0, r))

    lax.fori_loop(1, AHEAD, opening, 0)

    await_bytes(c_recv.at[pl.ds(1, MEMBERS - 1)], c_rs.at[0])
    group_count = c_send[0]
    for r in range(1, MEMBERS):
        group_count = group_count + c_recv[r]
    c_group[...] = group_count

    for h in (0, 1):
        z_send[h, 0, 3] = reduce_rows(0, h)
        forward(h, 0, 3)
    cz_send[0, 3] = count_of(4)
    forward_count(0, 3)

    def step(p, way, k, joined):
        for h in (0, 1):
            z_send[h, way, k] = reduce_rows(p, h)

            @pl.when(joined)
            def _():
                z_send[h, way, k] += incoming(h, way, k + 1)

            forward(h, way, k)
        count_step(way, k, joined)

    def count_step(way, k, joined):
        cz_send[way, k] = count_of(-k - 1 if way else k + 1)

        @pl.when(joined)
        def _():
            cz_send[way, k] += incoming_count(way, k + 1)

        forward_count(way, k)

    def pair(i, carry):
        k = 2 - i
        for way in (0, 1):
            p = 1 + 2 * i + way
            first(p + AHEAD - 1, 0)
            step(p, way, k, way == 0 or i > 0)
        return carry

    lax.fori_loop(0, 2, pair, 0)

    first(7, 0)
    step(5, 0, 0, True)
    onehots = [onehot_of(6, h) for h in (0, 1)]
    for h in (0, 1):
        await_bytes(z_recv.at[h, 1, 1], z_rs.at[h, 1, 1])
    for q in range(PIECES):
        for h in (0, 1):
            at = (h, 1, 0, slice(None), columns(q))
            z_send[at] = reduce_piece(onehots[h], 6, h, q) + z_recv[h, 1, 1, :, columns(q)]
            push(z_send.at[at], z_recv.at[at], last_ss.at[h, q], last_rs.at[h, q], onward(h, 1))
    count_step(1, 0, True)

    onehots = [onehot_of(7, h) for h in (0, 1)]
    for q in range(PIECES):
        for h in (0, 1):
            own = reduce_piece(onehots[h], 7, h, q)
            if q == 0:
                await_bytes(z_recv.at[h, 0, 0], z_rs.at[h, 0, 0])
            own = own + z_recv[h, 0, 0, :, columns(q)]
            await_bytes(z_recv.at[h, 1, 0, :, columns(q)], last_rs.at[h, q])
            own = own + z_recv[h, 1, 0, :, columns(q)]
            total[h, :, :, columns(q)] = own.reshape(4, OWN, PIECE)
            at = y if h == 0 else x
            for i in range(1, 4):
                push(
                    total.at[h, (at + i) % 4, :, columns(q)], part_recv.at[h, i, :, columns(q)],
                    part_ss.at[h, q], part_rs.at[h, q], other(h, i),
                )
        if q == 0:
            c_last[...] = count_of(0) + incoming_count(0, 0) + incoming_count(1, 0)
            for i in range(1, NY):
                push(c_last, c_last_recv.at[i], c_ss.at[1], c_rs.at[1], other(0, i))

    inputs[4].wait()
    await_bytes(c_last_recv.at[pl.ds(1, NY - 1)], c_rs.at[1])
    block_count = c_last[...]
    for i in range(1, NY):
        block_count = block_count + c_last_recv[i]
    for j in range(8):
        count_ref[j : j + 1, :] = block_count[:, j * 8 : (j + 1) * 8].astype(I32)
    own_sub = lax.broadcasted_iota(I32, (OWN, 128), 0) + y * OWN
    own_lane = lax.broadcasted_iota(I32, (OWN, 128), 1)
    column = jnp.sum(jnp.where(own_sub == own_lane, block_count, 0.0), axis=1, keepdims=True)

    for q in range(PIECES):
        for h in (0, 1):
            at = y if h == 0 else x
            cols = pl.ds(h * HALF + q * PIECE, PIECE)
            await_bytes(part_recv.at[h, pl.ds(1, 3), :, columns(q)], part_rs.at[h, q])
            mine = total[h, at, :, columns(q)]
            for i in range(1, 4):
                mine = mine + part_recv[h, i, :, columns(q)]
            old = old_ref[pl.ds(y * 2, 2), :, cols].reshape(OWN, PIECE)
            fresh[:, :, cols] = ((mine + old) / (column + 1.0)).reshape(2, 8, PIECE)
            src = fresh.at[:, :, cols]
            dst = out_ref.at[pl.ds(y * 2, 2), :, cols]
            for i in range(1, NY):
                push(src, dst, gather_ss.at[h, q], gather_rs.at[h, q], other(0, i))
            pltpu.make_async_copy(src, dst, own_sem.at[h, q]).start()

    for h in (0, 1):
        for p in range(8):
            await_bytes(lab_send.at[h, p, pl.ds(1, MEMBERS - 1)], lab_ss.at[h, p])
            if p < LATE:
                await_bytes(send.at[h, p, pl.ds(1, MEMBERS - 1)], data_ss.at[h, p])
        for way in (0, 1):
            for k in range(way, 4 - way):
                await_bytes(z_send.at[h, way, k], z_ss.at[h, way, k])
        for q in range(PIECES):
            for p in (6, 7):
                await_bytes(send.at[h, p, pl.ds(1, MEMBERS - 1), :, columns(q)], late_ss.at[h, p - LATE, q])
            await_bytes(z_send.at[h, 1, 0, :, columns(q)], last_ss.at[h, q])
            await_bytes(part_recv.at[h, pl.ds(1, 3), :, columns(q)], part_ss.at[h, q])
            cols = pl.ds(h * HALF + q * PIECE, PIECE)
            await_bytes(out_ref.at[pl.ds(0, 6), :, cols], gather_ss.at[h, q])
            await_bytes(out_ref.at[pl.ds(0, 6), :, cols], gather_rs.at[h, q])
            await_bytes(out_ref.at[pl.ds(0, 2), :, cols], own_sem.at[h, q])
    await_bytes(c_recv.at[pl.ds(1, MEMBERS - 1)], c_ss.at[0])
    await_bytes(c_last_recv.at[pl.ds(1, NY - 1)], c_ss.at[1])
    for way in (0, 1):
        for k in range(4 - way):
            await_bytes(cz_send.at[way, k], cz_ss.at[way, k])


def per_device(pool_rows, sample_index, cluster_id, child_id, old_centroids):
    vmem = pl.BlockSpec(memory_space=pltpu.VMEM)
    dma = pltpu.SemaphoreType.DMA
    centroids, counts = pl.pallas_call(
        kernel,
        out_shape=(
            jax.ShapeDtypeStruct((8, 8, WIDTH), F32),
            jax.ShapeDtypeStruct((8, 8), I32),
        ),
        in_specs=[pl.BlockSpec(memory_space=pltpu.HBM)] * 5,
        out_specs=(pl.BlockSpec(memory_space=pl.ANY), vmem),
        scratch_shapes=[
            pltpu.VMEM((ROWS, WIDTH), BF16),
            pltpu.VMEM((1, ROWS), I32),
            pltpu.VMEM((1, ROWS), I32),
            pltpu.VMEM((1, ROWS), I32),
            pltpu.VMEM((8, 8, WIDTH), F32),
            pltpu.VMEM((2, 1, ROWS), I32),
            pltpu.VMEM((ROWS, 128), BF16),
            pltpu.VMEM((2, 8, MEMBERS, SLOTS, HALF), BF16),
            pltpu.VMEM((2, 8, MEMBERS, SLOTS, HALF), BF16),
            pltpu.VMEM((2, 8, MEMBERS, 1, BLOCK), I32),
            pltpu.VMEM((2, 8, MEMBERS, 1, BLOCK), I32),
            pltpu.VMEM((2, 2, 4, SEGS, HALF), F32),
            pltpu.VMEM((2, 2, 4, SEGS, HALF), F32),
            pltpu.VMEM((2, 4, OWN, HALF), F32),
            pltpu.VMEM((2, 4, OWN, HALF), F32),
            pltpu.VMEM((2, 8, WIDTH), F32),
            pltpu.VMEM((MEMBERS, NZ, 128), F32),
            pltpu.VMEM((MEMBERS, NZ, 128), F32),
            pltpu.VMEM((NZ, 128), F32),
            pltpu.VMEM((2, 4, 1, 128), F32),
            pltpu.VMEM((2, 4, 1, 128), F32),
            pltpu.VMEM((1, 128), F32),
            pltpu.VMEM((NY, 1, 128), F32),
            dma((5,)), dma((2, 8)), dma((2, 8)), dma((2, 8)), dma((2, 8)),
            dma((2, 2, 4)), dma((2, 2, 4)), dma((2, PIECES)), dma((2, PIECES)),
            dma((2, PIECES)), dma((2, PIECES)), dma((2,)), dma((2,)), dma((2, 4)), dma((2, 4)),
            dma((2, PIECES)), dma((2, 2, PIECES)), dma((2, 2, PIECES)),
            dma((2, PIECES)), dma((2, PIECES)),
        ],
        compiler_params=pltpu.CompilerParams(
            collective_id=0, has_side_effects=True, vmem_limit_bytes=48 << 20
        ),
    )(
        *[
            pltpu.with_memory_space_constraint(a, pltpu.HBM)
            for a in (
                pool_rows,
                sample_index.reshape(1, ROWS),
                cluster_id.reshape(1, ROWS),
                child_id.reshape(1, ROWS),
                old_centroids,
            )
        ]
    )
    return centroids, counts


def solution(mesh):
    placed = (
        P(("grp", "dev"), None),
        P(("grp", "dev")),
        P(("grp", "dev")),
        P(("grp", "dev")),
        P("dev", None, None),
    )
    return jax.shard_map(
        per_device,
        mesh=mesh,
        in_specs=placed,
        out_specs=(P("dev", None, None), P("dev", None)),
        check_vma=False,
    )
```

```python
import jax
import jax.numpy as jnp
from jax import lax
from jax.experimental import pallas as pl
from jax.experimental.pallas import tpu as pltpu
from jax.sharding import PartitionSpec as P

MESH = pl.DeviceIdType.MESH
F32, BF16, I32 = jnp.float32, jnp.bfloat16, jnp.int32

NY, NX, NZ, NC = 4, 4, 8, 2
MEMBERS, SLOTS = 8, 32
BLOCK = MEMBERS * SLOTS
ROWS, WIDTH = 1024, 1024
HALF = WIDTH // 2
SEGS = 64
OWN = 16
AHEAD = 3
PIECES = 2
PIECE = HALF // PIECES
LATE = 6


def kernel(
    pool_hbm, index_hbm, cluster_hbm, child_hbm, old_hbm,
    out_ref, count_ref,
    pool_ref, index_ref, cluster_ref, child_ref, old_ref,
    slot_ref, values_ref, send, recv, lab_send, lab_recv,
    z_send, z_recv, total, part_recv, fresh,
    c_send, c_recv, c_group, cz_send, cz_recv, c_last, c_last_recv,
    in_sem, data_ss, data_rs, lab_ss, lab_rs, z_ss, z_rs, part_ss, part_rs,
    gather_ss, gather_rs, c_ss, c_rs, cz_ss, cz_rs, own_sem, late_ss, late_rs, last_ss, last_rs,
):
    y = lax.axis_index("grp")
    d = lax.axis_index("dev")
    x, z, c = d // (NZ * NC), (d // NC) % NZ, d % NC

    def dev(x_, z_, c_):
        return (x_ * NZ + z_) * NC + c_

    def member(h, r):
        e = ((x if h == 0 else y) * NC + c + r) % MEMBERS
        if h == 0:
            return (y, dev(e // NC, z, e % NC))
        return (e // NC, dev(x, z, e % NC))

    def along_z(step):
        return (y, dev(x, (z + step + NZ) % NZ, c))

    def other(h, i):
        if h == 0:
            return ((y + i) % NY, d)
        return (y, dev((x + i) % NX, z, c))

    def push(src, dst, ss, rs, to):
        pltpu.make_async_remote_copy(
            src_ref=src, dst_ref=dst, send_sem=ss, recv_sem=rs, device_id=to, device_id_type=MESH
        ).start()

    def await_bytes(ref, sem):
        pltpu.make_async_copy(ref, ref, sem).wait()

    inputs = [
        pltpu.make_async_copy(src, dst, in_sem.at[i])
        for i, (src, dst) in enumerate(
            [(index_hbm, index_ref), (cluster_hbm, cluster_ref), (child_hbm, child_ref),
             (pool_hbm, pool_ref), (old_hbm, old_ref)]
        )
    ]
    for copy in inputs:
        copy.start()

    barrier = pltpu.get_barrier_semaphore()
    greeted = [member(h, r) for h in (0, 1) for r in range(1, MEMBERS)]
    greeted += [along_z(1), along_z(-1)]
    for to in greeted:
        pl.semaphore_signal(barrier, inc=1, device_id=to, device_id_type=MESH)

    for copy in inputs[:3]:
        copy.wait()
    cluster, child = cluster_ref[...], child_ref[...]
    index = index_ref[...] & (ROWS - 1)
    cx, cz, cc, cj = cluster >> 7, (cluster >> 4) & 7, (cluster >> 3) & 1, cluster & 7

    def position(steps):
        near = jnp.where(steps < 4, 8 - 2 * steps, 2 * steps - 9)
        return jnp.where(steps == 0, 7, jnp.where(steps == 4, 0, near))

    zr = (cz - z + NZ) & (NZ - 1)
    pos_x = position(zr)
    zr = (NZ - zr) & (NZ - 1)
    pos_y = position(zr)
    rx = (cx * NC + cc - (x * NC + c) + MEMBERS) & (MEMBERS - 1)
    ry = ((cj >> 1) * NC + cc - (y * NC + c) + MEMBERS) & (MEMBERS - 1)
    label_x = cj * 8 + child
    label_y = cx * OWN + (cj & 1) * 8 + child
    cat_x = pos_x * MEMBERS + rx
    cat_y = pos_y * MEMBERS + ry + 64

    sub = lax.broadcasted_iota(I32, (128, 128), 0)
    lane = lax.broadcasted_iota(I32, (128, 128), 1)
    before = jnp.concatenate(
        [jnp.where(sub <= lane, 1.0, 0.0), jnp.ones((128, 128), F32)], axis=1
    ).astype(BF16)
    hits = []
    for b in range(ROWS // 128):
        at = slice(b * 128, (b + 1) * 128)
        hits.append((sub == cat_x[:, at]) | (sub == cat_y[:, at]))
    stacked = jnp.concatenate([jnp.where(m, 1.0, 0.0).astype(BF16) for m in hits], axis=0)
    ranks = jnp.dot(stacked, before, preferred_element_type=F32)
    base = ((sub & 63) * SLOTS - 1).astype(F32)
    for b in range(ROWS // 128):
        at = slice(b * 128, (b + 1) * 128)
        here = ranks[b * 128 : (b + 1) * 128]
        chosen = jnp.where(hits[b], here[:, :128] + base, 0.0)
        slot_ref[0, :, at] = jnp.sum(chosen[:64], axis=0, keepdims=True).astype(I32)
        slot_ref[1, :, at] = jnp.sum(chosen[64:], axis=0, keepdims=True).astype(I32)
        base = base + here[:, 128:]

    values = jnp.concatenate(
        [index >> 5, index & 31, label_x + 1, label_y + 1, jnp.zeros((4, ROWS), I32)], axis=0
    ).astype(F32)
    values = jnp.concatenate([values, jnp.zeros((120, ROWS), F32)], axis=0)
    values_ref[...] = values.T.astype(BF16)

    sub_block = lax.broadcasted_iota(I32, (BLOCK, ROWS), 0)
    lane_block = lax.broadcasted_iota(I32, (BLOCK, ROWS), 1)
    lab_lane = lax.broadcasted_iota(I32, (1, BLOCK), 1)

    def place(p, h):
        pick = jnp.where(sub_block == slot_ref[h] - p * BLOCK, 1.0, 0.0).astype(BF16)
        found = jnp.dot(pick, values_ref[...], preferred_element_type=F32)
        row = (found[:, 0:1] * 32.0 + found[:, 1:2]).astype(I32)
        labels = found.T[2 + h : 3 + h].astype(I32)
        take = jnp.where(lane_block == row, 1.0, 0.0).astype(BF16)
        rows = jnp.dot(
            take, pool_ref[:, h * HALF : (h + 1) * HALF], preferred_element_type=F32
        ).astype(BF16)
        recv[h, p, 0] = rows[:SLOTS]
        send[h, p, pl.ds(1, MEMBERS - 1)] = rows[SLOTS:].reshape(MEMBERS - 1, SLOTS, HALF)
        for r in range(MEMBERS):
            mine = jnp.where((lab_lane >> 5) == r, labels, 0)
            if r == 0:
                lab_recv[h, p, 0] = mine
            else:
                lab_send[h, p, r] = mine

    def columns(q):
        return pl.ds(q * PIECE, PIECE)

    def dispatch(p, h):
        for r in (2, 6, 4, 3, 7, 5, 1):
            to = member(h, r)
            push(lab_send.at[h, p, r], lab_recv.at[h, p, r], lab_ss.at[h, p], lab_rs.at[h, p], to)
            push(send.at[h, p, r], recv.at[h, p, r], data_ss.at[h, p], data_rs.at[h, p], to)

    def dispatch_pieces(p, h):
        for q in range(PIECES):
            for r in (2, 6, 4, 3, 7, 5, 1):
                to = member(h, r)
                if q == 0:
                    push(lab_send.at[h, p, r], lab_recv.at[h, p, r], lab_ss.at[h, p], lab_rs.at[h, p], to)
                at = (h, p - LATE, q)
                push(
                    send.at[h, p, r, :, columns(q)], recv.at[h, p, r, :, columns(q)],
                    late_ss.at[at], late_rs.at[at], to,
                )

    seg = lax.broadcasted_iota(I32, (SEGS, BLOCK), 0) + 1

    def onehot_of(p, h):
        await_bytes(lab_recv.at[h, p, pl.ds(1, MEMBERS - 1)], lab_rs.at[h, p])
        labels = lab_recv[h, p, 0]
        for r in range(1, MEMBERS):
            labels = labels + lab_recv[h, p, r]
        return jnp.where(seg == labels, 1.0, 0.0).astype(BF16)

    def reduce_rows(p, h):
        onehot = onehot_of(p, h)
        await_bytes(recv.at[h, p, pl.ds(1, MEMBERS - 1)], data_rs.at[h, p])
        return jnp.dot(onehot, recv[h, p].reshape(BLOCK, HALF), preferred_element_type=F32)

    def reduce_piece(onehot, p, h, q):
        await_bytes(recv.at[h, p, pl.ds(1, MEMBERS - 1), :, columns(q)], late_rs.at[h, p - LATE, q])
        rows = recv[h, p, :, :, columns(q)].reshape(BLOCK, PIECE)
        return jnp.dot(onehot, rows, preferred_element_type=F32)

    def onward(h, way):
        return along_z(1 if way == h else -1)

    def forward(h, way, k):
        push(
            z_send.at[h, way, k], z_recv.at[h, way, k], z_ss.at[h, way, k], z_rs.at[h, way, k],
            onward(h, way),
        )

    def incoming(h, way, k):
        await_bytes(z_recv.at[h, way, k], z_rs.at[h, way, k])
        return z_recv[h, way, k]

    def forward_count(way, k):
        push(
            cz_send.at[way, k], cz_recv.at[way, k], cz_ss.at[way, k], cz_rs.at[way, k],
            onward(0, way),
        )

    def incoming_count(way, k):
        await_bytes(cz_recv.at[way, k], cz_rs.at[way, k])
        return cz_recv[way, k]

    def count_of(steps):
        return c_group[pl.ds((z + steps + NZ) % NZ, 1), :]

    def first(p, carry):
        for h in (0, 1):
            place(p, h)

            @pl.when(p < LATE)
            def _():
                dispatch(p, h)

            @pl.when(p >= LATE)
            def _():
                dispatch_pieces(p, h)

        return carry

    def opening(p, carry):
        for h in (0, 1):
            place(p, h)
            dispatch(p, h)
        return carry

    inputs[3].wait()
    pl.semaphore_wait(barrier, len(greeted))
    lax.fori_loop(0, 1, opening, 0)

    place_row = rx * NZ + cz
    a_hot = jnp.where(lax.broadcasted_iota(I32, (64, ROWS), 0) == place_row, 1.0, 0.0).astype(BF16)
    b_hot = jnp.where(lax.broadcasted_iota(I32, (128, ROWS), 0) == label_x, 1.0, 0.0).astype(BF16)
    tally = lax.dot_general(a_hot, b_hot, (((1,), (1,)), ((), ())), preferred_element_type=F32)
    c_send[...] = tally.reshape(MEMBERS, NZ, 128)
    for r in range(1, MEMBERS):
        push(c_send.at[r], c_recv.at[r], c_ss.at[0], c_rs.at[0], member(0, r))

    lax.fori_loop(1, AHEAD, opening, 0)

    await_bytes(c_recv.at[pl.ds(1, MEMBERS - 1)], c_rs.at[0])
    group_count = c_send[0]
    for r in range(1, MEMBERS):
        group_count = group_count + c_recv[r]
    c_group[...] = group_count

    for h in (0, 1):
        z_send[h, 0, 3] = reduce_rows(0, h)
        forward(h, 0, 3)
    cz_send[0, 3] = count_of(4)
    forward_count(0, 3)

    def step(p, way, k, joined):
        for h in (0, 1):
            z_send[h, way, k] = reduce_rows(p, h)

            @pl.when(joined)
            def _():
                z_send[h, way, k] += incoming(h, way, k + 1)

            forward(h, way, k)
        count_step(way, k, joined)

    def count_step(way, k, joined):
        cz_send[way, k] = count_of(-k - 1 if way else k + 1)

        @pl.when(joined)
        def _():
            cz_send[way, k] += incoming_count(way, k + 1)

        forward_count(way, k)

    def pair(i, carry):
        k = 2 - i
        for way in (1, 0):
            p = 2 + 2 * i - way
            first(p + AHEAD - 1, 0)
            step(p, way, k, way == 0 or i > 0)
        return carry

    lax.fori_loop(0, 2, pair, 0)

    first(7, 0)
    step(5, 1, 0, True)
    onehots = [onehot_of(6, h) for h in (0, 1)]
    for h in (0, 1):
        await_bytes(z_recv.at[h, 0, 1], z_rs.at[h, 0, 1])
    for q in range(PIECES):
        for h in (0, 1):
            at = (h, 0, 0, slice(None), columns(q))
            z_send[at] = reduce_piece(onehots[h], 6, h, q) + z_recv[h, 0, 1, :, columns(q)]
            push(z_send.at[at], z_recv.at[at], last_ss.at[h, q], last_rs.at[h, q], onward(h, 0))
    count_step(0, 0, True)

    onehots = [onehot_of(7, h) for h in (0, 1)]
    for q in range(PIECES):
        for h in (0, 1):
            own = reduce_piece(onehots[h], 7, h, q)
            if q == 0:
                await_bytes(z_recv.at[h, 1, 0], z_rs.at[h, 1, 0])
            own = own + z_recv[h, 1, 0, :, columns(q)]
            await_bytes(z_recv.at[h, 0, 0, :, columns(q)], last_rs.at[h, q])
            own = own + z_recv[h, 0, 0, :, columns(q)]
            total[h, :, :, columns(q)] = own.reshape(4, OWN, PIECE)
            at = y if h == 0 else x
            for i in range(1, 4):
                push(
                    total.at[h, (at + i) % 4, :, columns(q)], part_recv.at[h, i, :, columns(q)],
                    part_ss.at[h, q], part_rs.at[h, q], other(h, i),
                )
        if q == 0:
            c_last[...] = count_of(0) + incoming_count(0, 0) + incoming_count(1, 0)
            for i in range(1, NY):
                push(c_last, c_last_recv.at[i], c_ss.at[1], c_rs.at[1], other(0, i))

    inputs[4].wait()
    await_bytes(c_last_recv.at[pl.ds(1, NY - 1)], c_rs.at[1])
    block_count = c_last[...]
    for i in range(1, NY):
        block_count = block_count + c_last_recv[i]
    for j in range(8):
        count_ref[j : j + 1, :] = block_count[:, j * 8 : (j + 1) * 8].astype(I32)
    own_sub = lax.broadcasted_iota(I32, (OWN, 128), 0) + y * OWN
    own_lane = lax.broadcasted_iota(I32, (OWN, 128), 1)
    column = jnp.sum(jnp.where(own_sub == own_lane, block_count, 0.0), axis=1, keepdims=True)

    for q in range(PIECES):
        for h in (0, 1):
            at = y if h == 0 else x
            cols = pl.ds(h * HALF + q * PIECE, PIECE)
            await_bytes(part_recv.at[h, pl.ds(1, 3), :, columns(q)], part_rs.at[h, q])
            mine = total[h, at, :, columns(q)]
            for i in range(1, 4):
                mine = mine + part_recv[h, i, :, columns(q)]
            old = old_ref[pl.ds(y * 2, 2), :, cols].reshape(OWN, PIECE)
            fresh[:, :, cols] = ((mine + old) / (column + 1.0)).reshape(2, 8, PIECE)
            src = fresh.at[:, :, cols]
            dst = out_ref.at[pl.ds(y * 2, 2), :, cols]
            for i in range(1, NY):
                push(src, dst, gather_ss.at[h, q], gather_rs.at[h, q], other(0, i))
            pltpu.make_async_copy(src, dst, own_sem.at[h, q]).start()

    for h in (0, 1):
        for p in range(8):
            await_bytes(lab_send.at[h, p, pl.ds(1, MEMBERS - 1)], lab_ss.at[h, p])
            if p < LATE:
                await_bytes(send.at[h, p, pl.ds(1, MEMBERS - 1)], data_ss.at[h, p])
        for way in (0, 1):
            for k in range(1 - way, 4 - way):
                await_bytes(z_send.at[h, way, k], z_ss.at[h, way, k])
        for q in range(PIECES):
            for p in (6, 7):
                await_bytes(send.at[h, p, pl.ds(1, MEMBERS - 1), :, columns(q)], late_ss.at[h, p - LATE, q])
            await_bytes(z_send.at[h, 0, 0, :, columns(q)], last_ss.at[h, q])
            await_bytes(part_recv.at[h, pl.ds(1, 3), :, columns(q)], part_ss.at[h, q])
            cols = pl.ds(h * HALF + q * PIECE, PIECE)
            await_bytes(out_ref.at[pl.ds(0, 6), :, cols], gather_ss.at[h, q])
            await_bytes(out_ref.at[pl.ds(0, 6), :, cols], gather_rs.at[h, q])
            await_bytes(out_ref.at[pl.ds(0, 2), :, cols], own_sem.at[h, q])
    await_bytes(c_recv.at[pl.ds(1, MEMBERS - 1)], c_ss.at[0])
    await_bytes(c_last_recv.at[pl.ds(1, NY - 1)], c_ss.at[1])
    for way in (0, 1):
        for k in range(4 - way):
            await_bytes(cz_send.at[way, k], cz_ss.at[way, k])


def per_device(pool_rows, sample_index, cluster_id, child_id, old_centroids):
    vmem = pl.BlockSpec(memory_space=pltpu.VMEM)
    dma = pltpu.SemaphoreType.DMA
    centroids, counts = pl.pallas_call(
        kernel,
        out_shape=(
            jax.ShapeDtypeStruct((8, 8, WIDTH), F32),
            jax.ShapeDtypeStruct((8, 8), I32),
        ),
        in_specs=[pl.BlockSpec(memory_space=pltpu.HBM)] * 5,
        out_specs=(pl.BlockSpec(memory_space=pl.ANY), vmem),
        scratch_shapes=[
            pltpu.VMEM((ROWS, WIDTH), BF16),
            pltpu.VMEM((1, ROWS), I32),
            pltpu.VMEM((1, ROWS), I32),
            pltpu.VMEM((1, ROWS), I32),
            pltpu.VMEM((8, 8, WIDTH), F32),
            pltpu.VMEM((2, 1, ROWS), I32),
            pltpu.VMEM((ROWS, 128), BF16),
            pltpu.VMEM((2, 8, MEMBERS, SLOTS, HALF), BF16),
            pltpu.VMEM((2, 8, MEMBERS, SLOTS, HALF), BF16),
            pltpu.VMEM((2, 8, MEMBERS, 1, BLOCK), I32),
            pltpu.VMEM((2, 8, MEMBERS, 1, BLOCK), I32),
            pltpu.VMEM((2, 2, 4, SEGS, HALF), F32),
            pltpu.VMEM((2, 2, 4, SEGS, HALF), F32),
            pltpu.VMEM((2, 4, OWN, HALF), F32),
            pltpu.VMEM((2, 4, OWN, HALF), F32),
            pltpu.VMEM((2, 8, WIDTH), F32),
            pltpu.VMEM((MEMBERS, NZ, 128), F32),
            pltpu.VMEM((MEMBERS, NZ, 128), F32),
            pltpu.VMEM((NZ, 128), F32),
            pltpu.VMEM((2, 4, 1, 128), F32),
            pltpu.VMEM((2, 4, 1, 128), F32),
            pltpu.VMEM((1, 128), F32),
            pltpu.VMEM((NY, 1, 128), F32),
            dma((5,)), dma((2, 8)), dma((2, 8)), dma((2, 8)), dma((2, 8)),
            dma((2, 2, 4)), dma((2, 2, 4)), dma((2, PIECES)), dma((2, PIECES)),
            dma((2, PIECES)), dma((2, PIECES)), dma((2,)), dma((2,)), dma((2, 4)), dma((2, 4)),
            dma((2, PIECES)), dma((2, 2, PIECES)), dma((2, 2, PIECES)),
            dma((2, PIECES)), dma((2, PIECES)),
        ],
        compiler_params=pltpu.CompilerParams(
            collective_id=0, has_side_effects=True, vmem_limit_bytes=48 << 20
        ),
    )(
        *[
            pltpu.with_memory_space_constraint(a, pltpu.HBM)
            for a in (
                pool_rows,
                sample_index.reshape(1, ROWS),
                cluster_id.reshape(1, ROWS),
                child_id.reshape(1, ROWS),
                old_centroids,
            )
        ]
    )
    return centroids, counts


def solution(mesh):
    placed = (
        P(("grp", "dev"), None),
        P(("grp", "dev")),
        P(("grp", "dev")),
        P(("grp", "dev")),
        P("dev", None, None),
    )
    return jax.shard_map(
        per_device,
        mesh=mesh,
        in_specs=placed,
        out_specs=(P("dev", None, None), P("dev", None)),
        check_vma=False,
    )
```

```python
import jax
import jax.numpy as jnp
from jax import lax
from jax.experimental import pallas as pl
from jax.experimental.pallas import tpu as pltpu
from jax.sharding import PartitionSpec as P

MESH = pl.DeviceIdType.MESH
F32, BF16, I32 = jnp.float32, jnp.bfloat16, jnp.int32

NY, NX, NZ, NC = 4, 4, 8, 2
MEMBERS, SLOTS = 8, 32
BLOCK = MEMBERS * SLOTS
ROWS, WIDTH = 1024, 1024
HALF = WIDTH // 2
SEGS = 64
OWN = 16
AHEAD = 3
PIECES = 2
PIECE = HALF // PIECES
LATE = 6


def kernel(
    pool_hbm, index_hbm, cluster_hbm, child_hbm, old_hbm,
    out_ref, count_ref,
    pool_ref, index_ref, cluster_ref, child_ref, old_ref,
    slot_ref, values_ref, send, recv, lab_send, lab_recv,
    z_send, z_recv, total, part_recv, fresh,
    c_send, c_recv, c_group, cz_send, cz_recv, c_last, c_last_recv,
    in_sem, data_ss, data_rs, lab_ss, lab_rs, z_ss, z_rs, part_ss, part_rs,
    gather_ss, gather_rs, c_ss, c_rs, cz_ss, cz_rs, own_sem, late_ss, late_rs, last_ss, last_rs,
):
    y = lax.axis_index("grp")
    d = lax.axis_index("dev")
    x, z, c = d // (NZ * NC), (d // NC) % NZ, d % NC

    def dev(x_, z_, c_):
        return (x_ * NZ + z_) * NC + c_

    def member(h, r):
        e = ((x if h == 0 else y) * NC + c + r) % MEMBERS
        if h == 0:
            return (y, dev(e // NC, z, e % NC))
        return (e // NC, dev(x, z, e % NC))

    def along_z(step):
        return (y, dev(x, (z + step + NZ) % NZ, c))

    def other(h, i):
        if h == 0:
            return ((y + i) % NY, d)
        return (y, dev((x + i) % NX, z, c))

    def push(src, dst, ss, rs, to):
        pltpu.make_async_remote_copy(
            src_ref=src, dst_ref=dst, send_sem=ss, recv_sem=rs, device_id=to, device_id_type=MESH
        ).start()

    def await_bytes(ref, sem):
        pltpu.make_async_copy(ref, ref, sem).wait()

    inputs = [
        pltpu.make_async_copy(src, dst, in_sem.at[i])
        for i, (src, dst) in enumerate(
            [(index_hbm, index_ref), (cluster_hbm, cluster_ref), (child_hbm, child_ref),
             (pool_hbm, pool_ref), (old_hbm, old_ref)]
        )
    ]
    for copy in inputs:
        copy.start()

    barrier = pltpu.get_barrier_semaphore()
    greeted = [member(h, r) for h in (0, 1) for r in range(1, MEMBERS)]
    greeted += [along_z(1), along_z(-1)]
    for to in greeted:
        pl.semaphore_signal(barrier, inc=1, device_id=to, device_id_type=MESH)

    for copy in inputs[:3]:
        copy.wait()
    cluster, child = cluster_ref[...], child_ref[...]
    index = index_ref[...] & (ROWS - 1)
    cx, cz, cc, cj = cluster >> 7, (cluster >> 4) & 7, (cluster >> 3) & 1, cluster & 7

    def position(steps):
        near = jnp.where(steps < 4, 8 - 2 * steps, 2 * steps - 9)
        return jnp.where(steps == 0, 7, jnp.where(steps == 4, 0, near))

    zr = (cz - z + NZ) & (NZ - 1)
    pos_x = position(zr)
    zr = (NZ - zr) & (NZ - 1)
    pos_y = position(zr)
    rx = (cx * NC + cc - (x * NC + c) + MEMBERS) & (MEMBERS - 1)
    ry = ((cj >> 1) * NC + cc - (y * NC + c) + MEMBERS) & (MEMBERS - 1)
    label_x = cj * 8 + child
    label_y = cx * OWN + (cj & 1) * 8 + child
    cat_x = pos_x * MEMBERS + rx
    cat_y = pos_y * MEMBERS + ry + 64

    sub = lax.broadcasted_iota(I32, (128, 128), 0)
    lane = lax.broadcasted_iota(I32, (128, 128), 1)
    before = jnp.concatenate(
        [jnp.where(sub <= lane, 1.0, 0.0), jnp.ones((128, 128), F32)], axis=1
    ).astype(BF16)
    hits = []
    for b in range(ROWS // 128):
        at = slice(b * 128, (b + 1) * 128)
        hits.append((sub == cat_x[:, at]) | (sub == cat_y[:, at]))
    stacked = jnp.concatenate([jnp.where(m, 1.0, 0.0).astype(BF16) for m in hits], axis=0)
    ranks = jnp.dot(stacked, before, preferred_element_type=F32)
    base = ((sub & 63) * SLOTS - 1).astype(F32)
    for b in range(ROWS // 128):
        at = slice(b * 128, (b + 1) * 128)
        here = ranks[b * 128 : (b + 1) * 128]
        chosen = jnp.where(hits[b], here[:, :128] + base, 0.0)
        slot_ref[0, :, at] = jnp.sum(chosen[:64], axis=0, keepdims=True).astype(I32)
        slot_ref[1, :, at] = jnp.sum(chosen[64:], axis=0, keepdims=True).astype(I32)
        base = base + here[:, 128:]

    values = jnp.concatenate(
        [index >> 5, index & 31, label_x + 1, label_y + 1, jnp.zeros((4, ROWS), I32)], axis=0
    ).astype(F32)
    values = jnp.concatenate([values, jnp.zeros((120, ROWS), F32)], axis=0)
    values_ref[...] = values.T.astype(BF16)

    sub_block = lax.broadcasted_iota(I32, (BLOCK, ROWS), 0)
    lane_block = lax.broadcasted_iota(I32, (BLOCK, ROWS), 1)
    lab_lane = lax.broadcasted_iota(I32, (1, BLOCK), 1)

    def place(p, h):
        pick = jnp.where(sub_block == slot_ref[h] - p * BLOCK, 1.0, 0.0).astype(BF16)
        found = jnp.dot(pick, values_ref[...], preferred_element_type=F32)
        row = (found[:, 0:1] * 32.0 + found[:, 1:2]).astype(I32)
        labels = found.T[2 + h : 3 + h].astype(I32)
        take = jnp.where(lane_block == row, 1.0, 0.0).astype(BF16)
        rows = jnp.dot(
            take, pool_ref[:, h * HALF : (h + 1) * HALF], preferred_element_type=F32
        ).astype(BF16)
        recv[h, p, 0] = rows[:SLOTS]
        send[h, p, pl.ds(1, MEMBERS - 1)] = rows[SLOTS:].reshape(MEMBERS - 1, SLOTS, HALF)
        for r in range(MEMBERS):
            mine = jnp.where((lab_lane >> 5) == r, labels, 0)
            if r == 0:
                lab_recv[h, p, 0] = mine
            else:
                lab_send[h, p, r] = mine

    def columns(q):
        return pl.ds(q * PIECE, PIECE)

    def dispatch(p, h):
        for r in (2, 6, 4, 3, 7, 5, 1):
            to = member(h, r)
            push(lab_send.at[h, p, r], lab_recv.at[h, p, r], lab_ss.at[h, p], lab_rs.at[h, p], to)
            push(send.at[h, p, r], recv.at[h, p, r], data_ss.at[h, p], data_rs.at[h, p], to)

    def dispatch_pieces(p, h):
        for q in range(PIECES):
            for r in (2, 6, 4, 3, 7, 5, 1):
                to = member(h, r)
                if q == 0:
                    push(lab_send.at[h, p, r], lab_recv.at[h, p, r], lab_ss.at[h, p], lab_rs.at[h, p], to)
                at = (h, p - LATE, q)
                push(
                    send.at[h, p, r, :, columns(q)], recv.at[h, p, r, :, columns(q)],
                    late_ss.at[at], late_rs.at[at], to,
                )

    seg = lax.broadcasted_iota(I32, (SEGS, BLOCK), 0) + 1

    def onehot_of(p, h):
        await_bytes(lab_recv.at[h, p, pl.ds(1, MEMBERS - 1)], lab_rs.at[h, p])
        labels = lab_recv[h, p, 0]
        for r in range(1, MEMBERS):
            labels = labels + lab_recv[h, p, r]
        return jnp.where(seg == labels, 1.0, 0.0).astype(BF16)

    def reduce_rows(p, h):
        onehot = onehot_of(p, h)
        await_bytes(recv.at[h, p, pl.ds(1, MEMBERS - 1)], data_rs.at[h, p])
        return jnp.dot(onehot, recv[h, p].reshape(BLOCK, HALF), preferred_element_type=F32)

    def reduce_piece(onehot, p, h, q):
        await_bytes(recv.at[h, p, pl.ds(1, MEMBERS - 1), :, columns(q)], late_rs.at[h, p - LATE, q])
        rows = recv[h, p, :, :, columns(q)].reshape(BLOCK, PIECE)
        return jnp.dot(onehot, rows, preferred_element_type=F32)

    def onward(h, way):
        return along_z(1 if way == h else -1)

    def forward(h, way, k):
        push(
            z_send.at[h, way, k], z_recv.at[h, way, k], z_ss.at[h, way, k], z_rs.at[h, way, k],
            onward(h, way),
        )

    def incoming(h, way, k):
        await_bytes(z_recv.at[h, way, k], z_rs.at[h, way, k])
        return z_recv[h, way, k]

    def forward_count(way, k):
        push(
            cz_send.at[way, k], cz_recv.at[way, k], cz_ss.at[way, k], cz_rs.at[way, k],
            onward(0, way),
        )

    def incoming_count(way, k):
        await_bytes(cz_recv.at[way, k], cz_rs.at[way, k])
        return cz_recv[way, k]

    def count_of(steps):
        return c_group[pl.ds((z + steps + NZ) % NZ, 1), :]

    def first(p, carry):
        for h in (0, 1):
            place(p, h)

            @pl.when(p < LATE)
            def _():
                dispatch(p, h)

            @pl.when(p >= LATE)
            def _():
                dispatch_pieces(p, h)

        return carry

    def opening(p, carry):
        for h in (0, 1):
            place(p, h)
            dispatch(p, h)
        return carry

    inputs[3].wait()
    pl.semaphore_wait(barrier, len(greeted))
    lax.fori_loop(0, 1, opening, 0)

    place_row = rx * NZ + cz
    a_hot = jnp.where(lax.broadcasted_iota(I32, (64, ROWS), 0) == place_row, 1.0, 0.0).astype(BF16)
    b_hot = jnp.where(lax.broadcasted_iota(I32, (128, ROWS), 0) == label_x, 1.0, 0.0).astype(BF16)
    tally = lax.dot_general(a_hot, b_hot, (((1,), (1,)), ((), ())), preferred_element_type=F32)
    c_send[...] = tally.reshape(MEMBERS, NZ, 128)
    for r in range(1, MEMBERS):
        push(c_send.at[r], c_recv.at[r], c_ss.at[0], c_rs.at[0], member(0, r))

    lax.fori_loop(1, AHEAD, opening, 0)

    await_bytes(c_recv.at[pl.ds(1, MEMBERS - 1)], c_rs.at[0])
    group_count = c_send[0]
    for r in range(1, MEMBERS):
        group_count = group_count + c_recv[r]
    c_group[...] = group_count

    for h in (0, 1):
        z_send[h, 0, 3] = reduce_rows(0, h)
        forward(h, 0, 3)
    cz_send[0, 3] = count_of(4)
    forward_count(0, 3)

    def step(p, way, k, joined):
        for h in (0, 1):
            z_send[h, way, k] = reduce_rows(p, h)

            @pl.when(joined)
            def _():
                z_send[h, way, k] += incoming(h, way, k + 1)

            forward(h, way, k)
        count_step(way, k, joined)

    def count_step(way, k, joined):
        cz_send[way, k] = count_of(-k - 1 if way else k + 1)

        @pl.when(joined)
        def _():
            cz_send[way, k] += incoming_count(way, k + 1)

        forward_count(way, k)

    def pair(i, carry):
        k = 2 - i
        for way in (1, 0):
            p = 2 + 2 * i - way
            first(p + AHEAD - 1, 0)
            step(p, way, k, way == 0 or i > 0)
        return carry

    lax.fori_loop(0, 2, pair, 0)

    first(7, 0)
    step(5, 1, 0, True)
    onehots = [onehot_of(6, h) for h in (0, 1)]
    for h in (0, 1):
        await_bytes(z_recv.at[h, 0, 1], z_rs.at[h, 0, 1])
    for q in range(PIECES):
        for h in (0, 1):
            at = (h, 0, 0, slice(None), columns(q))
            z_send[at] = reduce_piece(onehots[h], 6, h, q) + z_recv[h, 0, 1, :, columns(q)]
            push(z_send.at[at], z_recv.at[at], last_ss.at[h, q], last_rs.at[h, q], onward(h, 0))
    count_step(0, 0, True)

    onehots = [onehot_of(7, h) for h in (0, 1)]
    for q in range(PIECES):
        for h in (0, 1):
            own = reduce_piece(onehots[h], 7, h, q)
            if q == 0:
                await_bytes(z_recv.at[h, 1, 0], z_rs.at[h, 1, 0])
            own = own + z_recv[h, 1, 0, :, columns(q)]
            await_bytes(z_recv.at[h, 0, 0, :, columns(q)], last_rs.at[h, q])
            own = own + z_recv[h, 0, 0, :, columns(q)]
            total[h, :, :, columns(q)] = own.reshape(4, OWN, PIECE)
            at = y if h == 0 else x
            for i in range(1, 4):
                push(
                    total.at[h, (at + i) % 4, :, columns(q)], part_recv.at[h, i, :, columns(q)],
                    part_ss.at[h, q], part_rs.at[h, q], other(h, i),
                )
        if q == 0:
            c_last[...] = count_of(0) + incoming_count(0, 0) + incoming_count(1, 0)
            for i in range(1, NY):
                push(c_last, c_last_recv.at[i], c_ss.at[1], c_rs.at[1], other(0, i))

    inputs[4].wait()
    await_bytes(c_last_recv.at[pl.ds(1, NY - 1)], c_rs.at[1])
    block_count = c_last[...]
    for i in range(1, NY):
        block_count = block_count + c_last_recv[i]
    for j in range(8):
        count_ref[j : j + 1, :] = block_count[:, j * 8 : (j + 1) * 8].astype(I32)
    own_sub = lax.broadcasted_iota(I32, (OWN, 128), 0) + y * OWN
    own_lane = lax.broadcasted_iota(I32, (OWN, 128), 1)
    column = jnp.sum(jnp.where(own_sub == own_lane, block_count, 0.0), axis=1, keepdims=True)

    for q in range(PIECES):
        for h in (0, 1):
            at = y if h == 0 else x
            cols = pl.ds(h * HALF + q * PIECE, PIECE)
            await_bytes(part_recv.at[h, pl.ds(1, 3), :, columns(q)], part_rs.at[h, q])
            mine = total[h, at, :, columns(q)]
            for i in range(1, 4):
                mine = mine + part_recv[h, i, :, columns(q)]
            old = old_ref[pl.ds(y * 2, 2), :, cols].reshape(OWN, PIECE)
            fresh[:, :, cols] = ((mine + old) / (column + 1.0)).reshape(2, 8, PIECE)
            src = fresh.at[:, :, cols]
            dst = out_ref.at[pl.ds(y * 2, 2), :, cols]
            for i in range(1, NY):
                push(src, dst, gather_ss.at[h, q], gather_rs.at[h, q], other(0, i))
            pltpu.make_async_copy(src, dst, own_sem.at[h, q]).start()

    for h in (0, 1):
        for p in range(8):
            await_bytes(lab_send.at[h, p, pl.ds(1, MEMBERS - 1)], lab_ss.at[h, p])
            if p < LATE:
                await_bytes(send.at[h, p, pl.ds(1, MEMBERS - 1)], data_ss.at[h, p])
        for way in (0, 1):
            for k in range(1 - way, 4 - way):
                await_bytes(z_send.at[h, way, k], z_ss.at[h, way, k])
        for q in range(PIECES):
            for p in (6, 7):
                await_bytes(send.at[h, p, pl.ds(1, MEMBERS - 1), :, columns(q)], late_ss.at[h, p - LATE, q])
            await_bytes(z_send.at[h, 0, 0, :, columns(q)], last_ss.at[h, q])
            await_bytes(part_recv.at[h, pl.ds(1, 3), :, columns(q)], part_ss.at[h, q])
            cols = pl.ds(h * HALF + q * PIECE, PIECE)
            await_bytes(out_ref.at[pl.ds(0, 6), :, cols], gather_ss.at[h, q])
            await_bytes(out_ref.at[pl.ds(0, 6), :, cols], gather_rs.at[h, q])
            await_bytes(out_ref.at[pl.ds(0, 2), :, cols], own_sem.at[h, q])
    await_bytes(c_recv.at[pl.ds(1, MEMBERS - 1)], c_ss.at[0])
    await_bytes(c_last_recv.at[pl.ds(1, NY - 1)], c_ss.at[1])
    for way in (0, 1):
        for k in range(4 - way):
            await_bytes(cz_send.at[way, k], cz_ss.at[way, k])


def finish(centroids, counts, centroids_out, counts_out, sems):
    copies = [
        pltpu.make_async_copy(centroids, centroids_out, sems.at[0]),
        pltpu.make_async_copy(counts, counts_out, sems.at[1]),
    ]
    for copy in copies:
        copy.start()
    for copy in copies:
        copy.wait()


def per_device(pool_rows, sample_index, cluster_id, child_id, old_centroids):
    vmem = pl.BlockSpec(memory_space=pltpu.VMEM)
    dma = pltpu.SemaphoreType.DMA
    centroids, counts = pl.pallas_call(
        kernel,
        out_shape=(
            jax.ShapeDtypeStruct((8, 8, WIDTH), F32),
            jax.ShapeDtypeStruct((8, 8), I32),
        ),
        in_specs=[pl.BlockSpec(memory_space=pltpu.HBM)] * 5,
        out_specs=(pl.BlockSpec(memory_space=pl.ANY), vmem),
        scratch_shapes=[
            pltpu.VMEM((ROWS, WIDTH), BF16),
            pltpu.VMEM((1, ROWS), I32),
            pltpu.VMEM((1, ROWS), I32),
            pltpu.VMEM((1, ROWS), I32),
            pltpu.VMEM((8, 8, WIDTH), F32),
            pltpu.VMEM((2, 1, ROWS), I32),
            pltpu.VMEM((ROWS, 128), BF16),
            pltpu.VMEM((2, 8, MEMBERS, SLOTS, HALF), BF16),
            pltpu.VMEM((2, 8, MEMBERS, SLOTS, HALF), BF16),
            pltpu.VMEM((2, 8, MEMBERS, 1, BLOCK), I32),
            pltpu.VMEM((2, 8, MEMBERS, 1, BLOCK), I32),
            pltpu.VMEM((2, 2, 4, SEGS, HALF), F32),
            pltpu.VMEM((2, 2, 4, SEGS, HALF), F32),
            pltpu.VMEM((2, 4, OWN, HALF), F32),
            pltpu.VMEM((2, 4, OWN, HALF), F32),
            pltpu.VMEM((2, 8, WIDTH), F32),
            pltpu.VMEM((MEMBERS, NZ, 128), F32),
            pltpu.VMEM((MEMBERS, NZ, 128), F32),
            pltpu.VMEM((NZ, 128), F32),
            pltpu.VMEM((2, 4, 1, 128), F32),
            pltpu.VMEM((2, 4, 1, 128), F32),
            pltpu.VMEM((1, 128), F32),
            pltpu.VMEM((NY, 1, 128), F32),
            dma((5,)), dma((2, 8)), dma((2, 8)), dma((2, 8)), dma((2, 8)),
            dma((2, 2, 4)), dma((2, 2, 4)), dma((2, PIECES)), dma((2, PIECES)),
            dma((2, PIECES)), dma((2, PIECES)), dma((2,)), dma((2,)), dma((2, 4)), dma((2, 4)),
            dma((2, PIECES)), dma((2, 2, PIECES)), dma((2, 2, PIECES)),
            dma((2, PIECES)), dma((2, PIECES)),
        ],
        compiler_params=pltpu.CompilerParams(
            collective_id=0, has_side_effects=True, vmem_limit_bytes=48 << 20
        ),
    )(
        *[
            pltpu.with_memory_space_constraint(a, pltpu.HBM)
            for a in (
                pool_rows,
                sample_index.reshape(1, ROWS),
                cluster_id.reshape(1, ROWS),
                child_id.reshape(1, ROWS),
                old_centroids,
            )
        ]
    )
    return pl.pallas_call(
        finish,
        out_shape=(
            jax.ShapeDtypeStruct((8, 8, WIDTH), F32),
            jax.ShapeDtypeStruct((8, 8), I32),
        ),
        in_specs=[vmem] * 2,
        out_specs=(pl.BlockSpec(memory_space=pltpu.HBM),) * 2,
        scratch_shapes=[dma((2,))],
    )(*[pltpu.with_memory_space_constraint(a, pltpu.VMEM) for a in (centroids, counts)])


def solution(mesh):
    placed = (
        P(("grp", "dev"), None),
        P(("grp", "dev")),
        P(("grp", "dev")),
        P(("grp", "dev")),
        P("dev", None, None),
    )
    return jax.shard_map(
        per_device,
        mesh=mesh,
        in_specs=placed,
        out_specs=(P("dev", None, None), P("dev", None)),
        check_vma=False,
    )
```

```python
import jax
import jax.numpy as jnp
from jax import lax
from jax.experimental import pallas as pl
from jax.experimental.pallas import tpu as pltpu
from jax.sharding import PartitionSpec as P

MESH = pl.DeviceIdType.MESH
F32, BF16, I32 = jnp.float32, jnp.bfloat16, jnp.int32

NY, NX, NZ, NC = 4, 4, 8, 2
MEMBERS, SLOTS = 8, 32
BLOCK = MEMBERS * SLOTS
ROWS, WIDTH = 1024, 1024
HALF = WIDTH // 2
SEGS = 64
OWN = 16
AHEAD = 3
PIECES = 2
PIECE = HALF // PIECES
LATE = 6


def kernel(
    pool_hbm, index_hbm, cluster_hbm, child_hbm, old_hbm,
    out_ref, count_ref,
    pool_ref, index_ref, cluster_ref, child_ref, old_ref,
    slot_ref, values_ref, send, recv, lab_send, lab_recv,
    z_send, z_recv, total, part_recv, fresh,
    c_send, c_recv, c_group, cz_send, cz_recv, c_last, c_last_recv,
    in_sem, data_ss, data_rs, lab_ss, lab_rs, z_ss, z_rs, part_ss, part_rs,
    gather_ss, gather_rs, c_ss, c_rs, cz_ss, cz_rs, own_sem, late_ss, late_rs, last_ss, last_rs,
):
    y = lax.axis_index("grp")
    d = lax.axis_index("dev")
    x, z, c = d // (NZ * NC), (d // NC) % NZ, d % NC

    def dev(x_, z_, c_):
        return (x_ * NZ + z_) * NC + c_

    def member(h, r):
        e = ((x if h == 0 else y) * NC + c + r) % MEMBERS
        if h == 0:
            return (y, dev(e // NC, z, e % NC))
        return (e // NC, dev(x, z, e % NC))

    def along_z(step):
        return (y, dev(x, (z + step + NZ) % NZ, c))

    def other(h, i):
        if h == 0:
            return ((y + i) % NY, d)
        return (y, dev((x + i) % NX, z, c))

    def push(src, dst, ss, rs, to):
        pltpu.make_async_remote_copy(
            src_ref=src, dst_ref=dst, send_sem=ss, recv_sem=rs, device_id=to, device_id_type=MESH
        ).start()

    def await_bytes(ref, sem):
        pltpu.make_async_copy(ref, ref, sem).wait()

    inputs = [
        pltpu.make_async_copy(src, dst, in_sem.at[i])
        for i, (src, dst) in enumerate(
            [(index_hbm, index_ref), (cluster_hbm, cluster_ref), (child_hbm, child_ref),
             (pool_hbm, pool_ref), (old_hbm, old_ref)]
        )
    ]
    for copy in inputs:
        copy.start()

    barrier = pltpu.get_barrier_semaphore()
    greeted = [member(h, r) for h in (0, 1) for r in range(1, MEMBERS)]
    greeted += [along_z(1), along_z(-1)]
    for to in greeted:
        pl.semaphore_signal(barrier, inc=1, device_id=to, device_id_type=MESH)

    for copy in inputs[:3]:
        copy.wait()
    cluster, child = cluster_ref[...], child_ref[...]
    index = index_ref[...] & (ROWS - 1)
    cx, cz, cc, cj = cluster >> 7, (cluster >> 4) & 7, (cluster >> 3) & 1, cluster & 7

    def position(steps):
        near = jnp.where(steps < 4, 8 - 2 * steps, 2 * steps - 9)
        return jnp.where(steps == 0, 7, jnp.where(steps == 4, 0, near))

    zr = (cz - z + NZ) & (NZ - 1)
    pos_x = position(zr)
    zr = (NZ - zr) & (NZ - 1)
    pos_y = position(zr)
    rx = (cx * NC + cc - (x * NC + c) + MEMBERS) & (MEMBERS - 1)
    ry = ((cj >> 1) * NC + cc - (y * NC + c) + MEMBERS) & (MEMBERS - 1)
    label_x = cj * 8 + child
    label_y = cx * OWN + (cj & 1) * 8 + child
    cat_x = pos_x * MEMBERS + rx
    cat_y = pos_y * MEMBERS + ry + 64

    sub = lax.broadcasted_iota(I32, (128, 128), 0)
    lane = lax.broadcasted_iota(I32, (128, 128), 1)
    before = jnp.concatenate(
        [jnp.where(sub <= lane, 1.0, 0.0), jnp.ones((128, 128), F32)], axis=1
    ).astype(BF16)
    hits = []
    for b in range(ROWS // 128):
        at = slice(b * 128, (b + 1) * 128)
        hits.append((sub == cat_x[:, at]) | (sub == cat_y[:, at]))
    stacked = jnp.concatenate([jnp.where(m, 1.0, 0.0).astype(BF16) for m in hits], axis=0)
    ranks = jnp.dot(stacked, before, preferred_element_type=F32)
    base = ((sub & 63) * SLOTS - 1).astype(F32)
    for b in range(ROWS // 128):
        at = slice(b * 128, (b + 1) * 128)
        here = ranks[b * 128 : (b + 1) * 128]
        chosen = jnp.where(hits[b], here[:, :128] + base, 0.0)
        slot_ref[0, :, at] = jnp.sum(chosen[:64], axis=0, keepdims=True).astype(I32)
        slot_ref[1, :, at] = jnp.sum(chosen[64:], axis=0, keepdims=True).astype(I32)
        base = base + here[:, 128:]

    values = jnp.concatenate(
        [index >> 5, index & 31, label_x + 1, label_y + 1, jnp.zeros((4, ROWS), I32)], axis=0
    ).astype(F32)
    values = jnp.concatenate([values, jnp.zeros((120, ROWS), F32)], axis=0)
    values_ref[...] = values.T.astype(BF16)

    sub_block = lax.broadcasted_iota(I32, (BLOCK, ROWS), 0)
    lane_block = lax.broadcasted_iota(I32, (BLOCK, ROWS), 1)
    lab_lane = lax.broadcasted_iota(I32, (1, BLOCK // 2), 1)

    def place(p, h):
        pick = jnp.where(sub_block == slot_ref[h] - p * BLOCK, 1.0, 0.0).astype(BF16)
        found = jnp.dot(pick, values_ref[...], preferred_element_type=F32)
        row = (found[:, 0:1] * 32.0 + found[:, 1:2]).astype(I32)
        labels = found.T[2 + h : 3 + h].astype(I32)
        take = jnp.where(lane_block == row, 1.0, 0.0).astype(BF16)
        rows = jnp.dot(
            take, pool_ref[:, h * HALF : (h + 1) * HALF], preferred_element_type=F32
        ).astype(BF16)
        recv[h, p, 0] = rows[:SLOTS]
        send[h, p, pl.ds(1, MEMBERS - 1)] = rows[SLOTS:].reshape(MEMBERS - 1, SLOTS, HALF)
        for r in range(MEMBERS):
            half = labels[:, (r // 4) * 128 : (r // 4 + 1) * 128]
            mine = jnp.where((lab_lane >> 5) == r % 4, half, 0)
            if r == 0:
                lab_recv[h, p, 0] = mine
            else:
                lab_send[h, p, r] = mine

    def columns(q):
        return pl.ds(q * PIECE, PIECE)

    def dispatch(p, h):
        for r in (2, 6, 4, 3, 7, 5, 1):
            to = member(h, r)
            push(lab_send.at[h, p, r], lab_recv.at[h, p, r], lab_ss.at[h, p], lab_rs.at[h, p], to)
            push(send.at[h, p, r], recv.at[h, p, r], data_ss.at[h, p], data_rs.at[h, p], to)

    def dispatch_pieces(p, h):
        for q in range(PIECES):
            for r in (2, 6, 4, 3, 7, 5, 1):
                to = member(h, r)
                if q == 0:
                    push(lab_send.at[h, p, r], lab_recv.at[h, p, r], lab_ss.at[h, p], lab_rs.at[h, p], to)
                at = (h, p - LATE, q)
                push(
                    send.at[h, p, r, :, columns(q)], recv.at[h, p, r, :, columns(q)],
                    late_ss.at[at], late_rs.at[at], to,
                )

    seg = lax.broadcasted_iota(I32, (SEGS, BLOCK), 0) + 1

    def onehot_of(p, h):
        await_bytes(lab_recv.at[h, p, pl.ds(1, MEMBERS - 1)], lab_rs.at[h, p])
        low, high = lab_recv[h, p, 0], lab_recv[h, p, 4]
        for r in range(1, 4):
            low, high = low + lab_recv[h, p, r], high + lab_recv[h, p, 4 + r]
        labels = jnp.concatenate([low, high], axis=1)
        return jnp.where(seg == labels, 1.0, 0.0).astype(BF16)

    def reduce_rows(p, h):
        onehot = onehot_of(p, h)
        await_bytes(recv.at[h, p, pl.ds(1, MEMBERS - 1)], data_rs.at[h, p])
        return jnp.dot(onehot, recv[h, p].reshape(BLOCK, HALF), preferred_element_type=F32)

    def reduce_piece(onehot, p, h, q):
        await_bytes(recv.at[h, p, pl.ds(1, MEMBERS - 1), :, columns(q)], late_rs.at[h, p - LATE, q])
        rows = recv[h, p, :, :, columns(q)].reshape(BLOCK, PIECE)
        return jnp.dot(onehot, rows, preferred_element_type=F32)

    def onward(h, way):
        return along_z(1 if way == h else -1)

    def forward(h, way, k):
        push(
            z_send.at[h, way, k], z_recv.at[h, way, k], z_ss.at[h, way, k], z_rs.at[h, way, k],
            onward(h, way),
        )

    def incoming(h, way, k):
        await_bytes(z_recv.at[h, way, k], z_rs.at[h, way, k])
        return z_recv[h, way, k]

    def forward_count(way, k):
        push(
            cz_send.at[way, k], cz_recv.at[way, k], cz_ss.at[way, k], cz_rs.at[way, k],
            onward(0, way),
        )

    def incoming_count(way, k):
        await_bytes(cz_recv.at[way, k], cz_rs.at[way, k])
        return cz_recv[way, k]

    def count_of(steps):
        return c_group[pl.ds((z + steps + NZ) % NZ, 1), :]

    def first(p, carry):
        for h in (0, 1):
            place(p, h)

            @pl.when(p < LATE)
            def _():
                dispatch(p, h)

            @pl.when(p >= LATE)
            def _():
                dispatch_pieces(p, h)

        return carry

    def opening(p, carry):
        for h in (0, 1):
            place(p, h)
            dispatch(p, h)
        return carry

    inputs[3].wait()
    pl.semaphore_wait(barrier, len(greeted))
    lax.fori_loop(0, 1, opening, 0)

    place_row = rx * NZ + cz
    a_hot = jnp.where(lax.broadcasted_iota(I32, (64, ROWS), 0) == place_row, 1.0, 0.0).astype(BF16)
    b_hot = jnp.where(lax.broadcasted_iota(I32, (128, ROWS), 0) == label_x, 1.0, 0.0).astype(BF16)
    tally = lax.dot_general(a_hot, b_hot, (((1,), (1,)), ((), ())), preferred_element_type=F32)
    c_send[...] = tally.reshape(MEMBERS, NZ, 128)
    for r in range(1, MEMBERS):
        push(c_send.at[r], c_recv.at[r], c_ss.at[0], c_rs.at[0], member(0, r))

    lax.fori_loop(1, AHEAD, opening, 0)

    await_bytes(c_recv.at[pl.ds(1, MEMBERS - 1)], c_rs.at[0])
    group_count = c_send[0]
    for r in range(1, MEMBERS):
        group_count = group_count + c_recv[r]
    c_group[...] = group_count

    for h in (0, 1):
        z_send[h, 0, 3] = reduce_rows(0, h)
        forward(h, 0, 3)
    cz_send[0, 3] = count_of(4)
    forward_count(0, 3)

    def step(p, way, k, joined):
        for h in (0, 1):
            z_send[h, way, k] = reduce_rows(p, h)

            @pl.when(joined)
            def _():
                z_send[h, way, k] += incoming(h, way, k + 1)

            forward(h, way, k)
        count_step(way, k, joined)

    def count_step(way, k, joined):
        cz_send[way, k] = count_of(-k - 1 if way else k + 1)

        @pl.when(joined)
        def _():
            cz_send[way, k] += incoming_count(way, k + 1)

        forward_count(way, k)

    def pair(i, carry):
        k = 2 - i
        for way in (1, 0):
            p = 2 + 2 * i - way
            first(p + AHEAD - 1, 0)
            step(p, way, k, way == 0 or i > 0)
        return carry

    lax.fori_loop(0, 2, pair, 0)

    first(7, 0)
    step(5, 1, 0, True)
    onehots = [onehot_of(6, h) for h in (0, 1)]
    for h in (0, 1):
        await_bytes(z_recv.at[h, 0, 1], z_rs.at[h, 0, 1])
    for q in range(PIECES):
        for h in (0, 1):
            at = (h, 0, 0, slice(None), columns(q))
            z_send[at] = reduce_piece(onehots[h], 6, h, q) + z_recv[h, 0, 1, :, columns(q)]
            push(z_send.at[at], z_recv.at[at], last_ss.at[h, q], last_rs.at[h, q], onward(h, 0))
    count_step(0, 0, True)

    onehots = [onehot_of(7, h) for h in (0, 1)]
    for q in range(PIECES):
        for h in (0, 1):
            own = reduce_piece(onehots[h], 7, h, q)
            if q == 0:
                await_bytes(z_recv.at[h, 1, 0], z_rs.at[h, 1, 0])
            own = own + z_recv[h, 1, 0, :, columns(q)]
            await_bytes(z_recv.at[h, 0, 0, :, columns(q)], last_rs.at[h, q])
            own = own + z_recv[h, 0, 0, :, columns(q)]
            total[h, :, :, columns(q)] = own.reshape(4, OWN, PIECE)
            at = y if h == 0 else x
            for i in range(1, 4):
                push(
                    total.at[h, (at + i) % 4, :, columns(q)], part_recv.at[h, i, :, columns(q)],
                    part_ss.at[h, q], part_rs.at[h, q], other(h, i),
                )
        if q == 0:
            c_last[...] = count_of(0) + incoming_count(0, 0) + incoming_count(1, 0)
            for i in range(1, NY):
                push(c_last, c_last_recv.at[i], c_ss.at[1], c_rs.at[1], other(0, i))

    inputs[4].wait()
    await_bytes(c_last_recv.at[pl.ds(1, NY - 1)], c_rs.at[1])
    block_count = c_last[...]
    for i in range(1, NY):
        block_count = block_count + c_last_recv[i]
    for j in range(8):
        count_ref[j : j + 1, :] = block_count[:, j * 8 : (j + 1) * 8].astype(I32)
    own_sub = lax.broadcasted_iota(I32, (OWN, 128), 0) + y * OWN
    own_lane = lax.broadcasted_iota(I32, (OWN, 128), 1)
    column = jnp.sum(jnp.where(own_sub == own_lane, block_count, 0.0), axis=1, keepdims=True)

    for q in range(PIECES):
        for h in (0, 1):
            at = y if h == 0 else x
            cols = pl.ds(h * HALF + q * PIECE, PIECE)
            await_bytes(part_recv.at[h, pl.ds(1, 3), :, columns(q)], part_rs.at[h, q])
            mine = total[h, at, :, columns(q)]
            for i in range(1, 4):
                mine = mine + part_recv[h, i, :, columns(q)]
            old = old_ref[pl.ds(y * 2, 2), :, cols].reshape(OWN, PIECE)
            fresh[:, :, cols] = ((mine + old) / (column + 1.0)).reshape(2, 8, PIECE)
            src = fresh.at[:, :, cols]
            dst = out_ref.at[pl.ds(y * 2, 2), :, cols]
            for i in range(1, NY):
                push(src, dst, gather_ss.at[h, q], gather_rs.at[h, q], other(0, i))
            pltpu.make_async_copy(src, dst, own_sem.at[h, q]).start()

    for h in (0, 1):
        for p in range(8):
            await_bytes(lab_send.at[h, p, pl.ds(1, MEMBERS - 1)], lab_ss.at[h, p])
            if p < LATE:
                await_bytes(send.at[h, p, pl.ds(1, MEMBERS - 1)], data_ss.at[h, p])
        for way in (0, 1):
            for k in range(1 - way, 4 - way):
                await_bytes(z_send.at[h, way, k], z_ss.at[h, way, k])
        for q in range(PIECES):
            for p in (6, 7):
                await_bytes(send.at[h, p, pl.ds(1, MEMBERS - 1), :, columns(q)], late_ss.at[h, p - LATE, q])
            await_bytes(z_send.at[h, 0, 0, :, columns(q)], last_ss.at[h, q])
            await_bytes(part_recv.at[h, pl.ds(1, 3), :, columns(q)], part_ss.at[h, q])
            cols = pl.ds(h * HALF + q * PIECE, PIECE)
            await_bytes(out_ref.at[pl.ds(0, 6), :, cols], gather_ss.at[h, q])
            await_bytes(out_ref.at[pl.ds(0, 6), :, cols], gather_rs.at[h, q])
            await_bytes(out_ref.at[pl.ds(0, 2), :, cols], own_sem.at[h, q])
    await_bytes(c_recv.at[pl.ds(1, MEMBERS - 1)], c_ss.at[0])
    await_bytes(c_last_recv.at[pl.ds(1, NY - 1)], c_ss.at[1])
    for way in (0, 1):
        for k in range(4 - way):
            await_bytes(cz_send.at[way, k], cz_ss.at[way, k])


def finish(centroids, counts, centroids_out, counts_out, sems):
    copies = [
        pltpu.make_async_copy(centroids, centroids_out, sems.at[0]),
        pltpu.make_async_copy(counts, counts_out, sems.at[1]),
    ]
    for copy in copies:
        copy.start()
    for copy in copies:
        copy.wait()


def per_device(pool_rows, sample_index, cluster_id, child_id, old_centroids):
    vmem = pl.BlockSpec(memory_space=pltpu.VMEM)
    dma = pltpu.SemaphoreType.DMA
    centroids, counts = pl.pallas_call(
        kernel,
        out_shape=(
            jax.ShapeDtypeStruct((8, 8, WIDTH), F32),
            jax.ShapeDtypeStruct((8, 8), I32),
        ),
        in_specs=[pl.BlockSpec(memory_space=pltpu.HBM)] * 5,
        out_specs=(pl.BlockSpec(memory_space=pl.ANY), vmem),
        scratch_shapes=[
            pltpu.VMEM((ROWS, WIDTH), BF16),
            pltpu.VMEM((1, ROWS), I32),
            pltpu.VMEM((1, ROWS), I32),
            pltpu.VMEM((1, ROWS), I32),
            pltpu.VMEM((8, 8, WIDTH), F32),
            pltpu.VMEM((2, 1, ROWS), I32),
            pltpu.VMEM((ROWS, 128), BF16),
            pltpu.VMEM((2, 8, MEMBERS, SLOTS, HALF), BF16),
            pltpu.VMEM((2, 8, MEMBERS, SLOTS, HALF), BF16),
            pltpu.VMEM((2, 8, MEMBERS, 1, BLOCK // 2), I32),
            pltpu.VMEM((2, 8, MEMBERS, 1, BLOCK // 2), I32),
            pltpu.VMEM((2, 2, 4, SEGS, HALF), F32),
            pltpu.VMEM((2, 2, 4, SEGS, HALF), F32),
            pltpu.VMEM((2, 4, OWN, HALF), F32),
            pltpu.VMEM((2, 4, OWN, HALF), F32),
            pltpu.VMEM((2, 8, WIDTH), F32),
            pltpu.VMEM((MEMBERS, NZ, 128), F32),
            pltpu.VMEM((MEMBERS, NZ, 128), F32),
            pltpu.VMEM((NZ, 128), F32),
            pltpu.VMEM((2, 4, 1, 128), F32),
            pltpu.VMEM((2, 4, 1, 128), F32),
            pltpu.VMEM((1, 128), F32),
            pltpu.VMEM((NY, 1, 128), F32),
            dma((5,)), dma((2, 8)), dma((2, 8)), dma((2, 8)), dma((2, 8)),
            dma((2, 2, 4)), dma((2, 2, 4)), dma((2, PIECES)), dma((2, PIECES)),
            dma((2, PIECES)), dma((2, PIECES)), dma((2,)), dma((2,)), dma((2, 4)), dma((2, 4)),
            dma((2, PIECES)), dma((2, 2, PIECES)), dma((2, 2, PIECES)),
            dma((2, PIECES)), dma((2, PIECES)),
        ],
        compiler_params=pltpu.CompilerParams(
            collective_id=0, has_side_effects=True, vmem_limit_bytes=48 << 20
        ),
    )(
        *[
            pltpu.with_memory_space_constraint(a, pltpu.HBM)
            for a in (
                pool_rows,
                sample_index.reshape(1, ROWS),
                cluster_id.reshape(1, ROWS),
                child_id.reshape(1, ROWS),
                old_centroids,
            )
        ]
    )
    return pl.pallas_call(
        finish,
        out_shape=(
            jax.ShapeDtypeStruct((8, 8, WIDTH), F32),
            jax.ShapeDtypeStruct((8, 8), I32),
        ),
        in_specs=[vmem] * 2,
        out_specs=(pl.BlockSpec(memory_space=pltpu.HBM),) * 2,
        scratch_shapes=[dma((2,))],
    )(*[pltpu.with_memory_space_constraint(a, pltpu.VMEM) for a in (centroids, counts)])


def solution(mesh):
    placed = (
        P(("grp", "dev"), None),
        P(("grp", "dev")),
        P(("grp", "dev")),
        P(("grp", "dev")),
        P("dev", None, None),
    )
    return jax.shard_map(
        per_device,
        mesh=mesh,
        in_specs=placed,
        out_specs=(P("dev", None, None), P("dev", None)),
        check_vma=False,
    )
```
